128 devices in a mesh: chain: 64 (over z, x_hi, y, core), aux: 2 (over x_lo).
Axes of the slice: x: 4 (x_hi: 2, x_lo: 2; x = x_hi * 2 + x_lo), y: 4, z: 4, core: 2. Of those that a mesh axis runs over, the one named last changes fastest.
Arguments:
- occupied: bfloat16 [8192, 1152], P('chain'), may hold values from -0.1875 to 0.1875
- virtual: bfloat16 [8192, 1152], P('chain'), may hold values from -0.1875 to 0.1875
- three_centre: bfloat16 [32, 8192, 1152], P('aux', 'chain'), may hold values from -6 to 6
- kernel: bfloat16 [32, 32], P('aux'), may hold values from -1 to 1
- profile: int32 [64], replicated, may hold values from 2 to 4
- atom_map: int32 [32], P('aux'), may hold values from 0 to 63
Outputs:
- band_gradient: float32 [8192, 1152], P(('chain', 'aux'))
- polarization: float32 [32, 32], P('aux')
The draws below stay inside these ranges and needn't reach their ends.
All inputs are finite; a program needn't handle non-finite values.
Results may differ from the reference program's by a relative error of at most 0.0042.
Values may be sent and summed in bfloat16 or wider, within the bound.
A program may use at most 128 MiB of HBM per device.

```python
import math
import jax
import jax.numpy as jnp
from jax import lax

BLOCK = 128
BAND = 4
NBLK = 64
NBAS = 8192
NAUX = 32
BANDW = 1152
REACH = 16


def with_ends(values, stream_key, smallest, largest):
    extent = values.shape
    index_at = [jax.random.randint(jax.random.fold_in(stream_key, axis), (), 0, extent[axis]) for axis in range(len(extent))]
    values = values.at[tuple(index_at)].set(smallest)
    longest = extent.index(max(extent))
    index_at[longest] = (index_at[longest] + 1) % extent[longest]
    return values.at[tuple(index_at)].set(largest)


def levels(own_key, shape, split, smallest, top_value):
    level = 1.0
    for axis_at, shards_of in split:
        heights = jax.random.uniform(jax.random.fold_in(jax.random.fold_in(own_key, 6), axis_at), (shards_of,), jnp.float32, smallest / len(split), top_value / len(split))
        level = level * jnp.repeat(jnp.exp(heights), shape[axis_at] // shards_of).reshape((-1,) + (1,) * (len(shape) - 1 - axis_at))
    return level


def gaussian(key, shape, spread, bound, split=(), held_as=jnp.bfloat16):
    gain = levels(key, shape, split, -0.22, 0.18) if split else 1.0
    result = jax.random.normal(key, shape, jnp.float32) * spread * gain
    return jnp.minimum(jnp.maximum(result, -bound), bound).astype(held_as)


def setup_inputs(seed: int = 0) -> dict:
    keys = jax.random.split(jax.random.key(seed), 7)
    return {
        "occupied": gaussian(keys[0], (NBAS, BANDW), BANDW ** -0.5, 0.1875, ((0, 64),)),
        "virtual": gaussian(keys[1], (NBAS, BANDW), BANDW ** -0.5, 0.1875, ((0, 64),)),
        "three_centre": gaussian(keys[2], (NAUX, NBAS, BANDW), 1.0, 6.0, ((0, 2), (1, 64))),
        "kernel": gaussian(keys[3], (NAUX, NAUX), NAUX ** -0.5, 1.0, ((0, 2),)),
        "profile": with_ends(jax.random.randint(keys[4], (NBLK,), 2, BAND + 1), jax.random.fold_in(keys[4], 1), 2, BAND).astype(jnp.int32),
        "atom_map": with_ends(jax.random.randint(keys[5], (NAUX,), 0, NBLK), jax.random.fold_in(keys[5], 1), 0, NBLK - 1).astype(jnp.int32),
    }


def shift_blocks(matrix, offset, block_size):
    if offset == 0:
        return matrix
    padding = jnp.zeros(matrix.shape[:-1] + (abs(offset) * block_size,), matrix.dtype)
    if offset > 0:
        return jnp.concatenate([padding, matrix[..., :-offset * block_size]], -1)
    return jnp.concatenate([matrix[..., -offset * block_size:], padding], -1)

def reference(occupied, virtual, three_centre, kernel, profile, atom_map):
    slots_total = 2 * BAND + 1
    indices = jnp.arange(NBLK, dtype=jnp.int32)
    padded_profile = jnp.pad(profile, BAND)
    neighbours = jnp.stack([padded_profile[slot_index:slot_index + NBLK] for slot_index in range(slots_total)], 1)
    distance = jnp.abs(jnp.arange(slots_total, dtype=jnp.int32) - BAND)
    allowed = distance[None, :] <= jnp.minimum(profile[:, None], neighbours)
    column_mask = jnp.repeat(allowed, BLOCK, axis=1)
    zero_half = jnp.zeros((), jnp.bfloat16)
    occ_rows = jnp.where(column_mask[:, None, :], occupied.reshape(NBLK, BLOCK, BANDW), zero_half)
    vir_rows = jnp.where(column_mask[:, None, :], virtual.reshape(NBLK, BLOCK, BANDW), zero_half)
    occ_padded = jnp.pad(occ_rows, ((BAND, BAND), (0, 0), (0, 0)))
    vir_padded = jnp.pad(vir_rows, ((BAND, BAND), (0, 0), (0, 0)))
    integrals = three_centre.reshape(NAUX, NBLK, BLOCK, BANDW)
    screen = jnp.abs(atom_map[:, None] - indices[None, :]) <= REACH

    def per_block(state_pair, block_index):
        gradient_pad, polar_sum = state_pair
        near_occ = lax.dynamic_slice_in_dim(occ_padded, block_index, slots_total, 0)
        near_vir = lax.dynamic_slice_in_dim(vir_padded, block_index, slots_total, 0)
        stack_occ = jnp.concatenate([shift_blocks(near_occ[k], k - BAND, BLOCK) for k in range(slots_total)], 0)
        stack_vir = jnp.concatenate([shift_blocks(near_vir[k], k - BAND, BLOCK) for k in range(slots_total)], 0)
        local = lax.dynamic_index_in_dim(integrals, block_index, 1, keepdims=False)
        col_keep = lax.dynamic_index_in_dim(column_mask, block_index, 0, keepdims=False)
        aux_keep = lax.dynamic_index_in_dim(screen, block_index, 1, keepdims=False)
        local = jnp.where(col_keep[None, None, :] & aux_keep[:, None, None], local, zero_half)
        screened = local.reshape(NAUX * BLOCK, BANDW)
        coupled = jnp.dot(screened, stack_occ, preferred_element_type=jnp.float32).astype(jnp.bfloat16)
        partner = jnp.dot(screened, stack_vir, preferred_element_type=jnp.float32).astype(jnp.bfloat16)
        coupled_rows = coupled.reshape(NAUX, BLOCK * BANDW)
        partner_rows = partner.reshape(NAUX, BLOCK * BANDW)
        polar_sum = polar_sum + jnp.dot(coupled_rows, partner_rows.T, preferred_element_type=jnp.float32)
        response = jnp.dot(kernel, partner_rows, preferred_element_type=jnp.float32).astype(jnp.bfloat16)
        partials = lax.dot_general(screened, response.reshape(NAUX * BLOCK, BANDW), (((0,), (0,)), ((), ())), preferred_element_type=jnp.float32)
        partials = partials.reshape(slots_total, BLOCK, BANDW)
        moved = jnp.stack([shift_blocks(partials[k], BAND - k, BLOCK) for k in range(slots_total)], 0)
        current = lax.dynamic_slice_in_dim(gradient_pad, block_index, slots_total, 0)
        gradient_pad = lax.dynamic_update_slice_in_dim(gradient_pad, current + moved, block_index, 0)
        return ((gradient_pad, polar_sum), None)
    initial = (jnp.zeros((NBLK + 2 * BAND, BLOCK, BANDW), jnp.float32), jnp.zeros((NAUX, NAUX), jnp.float32))
    (gradient_pad, polar_sum), unused = lax.scan(per_block, initial, indices)
    scale_grad = 1.0 / math.sqrt(BLOCK * NAUX)
    scale_pol = 1.0 / math.sqrt(NBAS * BANDW)
    gradient = jnp.where(column_mask[:, None, :], gradient_pad[BAND:BAND + NBLK], jnp.zeros((), jnp.float32)) * scale_grad
    return (gradient.reshape(NBAS, BANDW), polar_sum * scale_pol)
```

```python
import functools
import math

import jax
import jax.numpy as jnp
from jax import lax
from jax.experimental import pallas as pl
from jax.experimental.pallas import tpu as pltpu
from jax.sharding import PartitionSpec as P

MESH = pl.DeviceIdType.MESH
BF16 = jnp.bfloat16
F32 = jnp.float32
B = 128
SLOTS = 9
W = SLOTS * B
ROWS = 16
TILES = ((0, 2, 0, 6), (2, 4, 0, 8), (4, 6, 0, 9), (6, 8, 2, 9))

S_IN = 0
UP1, DOWN1, UP2, DOWN2 = 4, 5, 6, 7
PAIR = 8
INFO = 12
GPAIR = 13
GUP2, GDOWN2, GUP1, GDOWN1 = 17, 18, 19, 20
GAUX = 21
POLAR = 22


def kernel(
    nchain,
    naux,
    reach,
    scale_grad,
    scale_pol,
    occ_hbm,
    vir_hbm,
    tc_hbm,
    kern_ref,
    profile_ref,
    atom_ref,
    grad_ref,
    pol_ref,
    s_buf,
    halo,
    pair_halo,
    x_buf,
    v_buf,
    xv_last,
    s_t,
    coupled,
    partner,
    response,
    gram,
    kron,
    info,
    terms,
    pair_out,
    pair_in,
    out2,
    in2,
    out1,
    in1,
    total,
    aux_out,
    aux_in,
    pol_out,
    pol_in,
    send_sem,
    recv_sem,
    local_sem,
):
    half = naux // 2
    chunks = (B // 2) // ROWS
    rounds = int(math.log2(nchain)) + 1
    chips = nchain // 2
    ci = lax.axis_index("chain")
    a = lax.axis_index("aux")
    chip = lax.div(ci, 2)
    core = lax.rem(ci, 2)
    inrow = lax.rem(chip, 4)
    flip_up = lax.div(inrow + 1, 4)
    flip_down = 1 - lax.div(inrow + 3, 4)
    up = (2 * lax.rem(chip + 1, chips) + core, lax.rem(a + flip_up, 2))
    down = (2 * lax.rem(chip + chips - 1, chips) + core, lax.rem(a + flip_down, 2))
    mate = (2 * chip + 1 - core, a)
    twin = (ci, 1 - a)

    def across(bit):
        size = 1 << bit
        return (ci + size * (1 - 2 * lax.rem(lax.div(ci, size), 2)), a)

    polar_peers = [mate, twin] + [across(bit) for bit in range(1, rounds - 1)]

    def remote(src, dst, number, device):
        return pltpu.make_async_remote_copy(
            src_ref=src,
            dst_ref=dst,
            send_sem=send_sem.at[number],
            recv_sem=recv_sem.at[number],
            device_id=device,
            device_id_type=MESH,
        )

    own_copies = [
        pltpu.make_async_copy(occ_hbm, halo.at[2, 0], local_sem.at[0]),
        pltpu.make_async_copy(vir_hbm, halo.at[2, 1], local_sem.at[1]),
    ]
    slab_copies = [
        pltpu.make_async_copy(
            tc_hbm.at[:, chunks * a + g], s_buf.at[g, pl.ds(half * a, half)], local_sem.at[2 + g]
        )
        for g in range(chunks)
    ]
    for copy in own_copies + slab_copies:
        copy.start()

    pair_in[...] = jnp.zeros_like(pair_in)
    row_id = lax.broadcasted_iota(jnp.int32, (half, B), 0)
    screen = jnp.zeros((half, B), F32)
    for p in range(half):
        near = jnp.abs(atom_ref[p] - ci) <= reach
        screen = jnp.where(row_id == p, jnp.where(near, 1.0, 0.0).astype(F32), screen)
    info[a, 0] = jnp.zeros((half, B), F32)
    info[a, 0, :, pl.ds(0, naux)] = kern_ref[...].astype(F32)
    info[a, 1] = screen

    barrier = pltpu.get_barrier_semaphore()
    greeted = [up, down] + polar_peers
    for device in greeted:
        pl.semaphore_signal(barrier, inc=1, device_id=device, device_id_type=MESH)
    pl.semaphore_wait(barrier, len(greeted))

    info_copy = remote(info.at[a], info.at[a], INFO, twin)
    info_copy.start()
    for g in range(chunks):
        remote(
            tc_hbm.at[:, chunks * (1 - a) + g],
            s_buf.at[g, pl.ds(half * a, half)],
            S_IN + g,
            twin,
        ).start()
    for copy in own_copies:
        copy.wait()
    up1 = remote(halo.at[2, :, :, pl.ds(B, 8 * B)], halo.at[1, :, :, pl.ds(B, 8 * B)], UP1, up)
    down1 = remote(halo.at[2, :, :, pl.ds(0, 8 * B)], halo.at[3, :, :, pl.ds(0, 8 * B)], DOWN1, down)
    up1.start()
    down1.start()
    up2 = remote(halo.at[1, :, :, pl.ds(3 * B, 6 * B)], halo.at[0, :, :, pl.ds(3 * B, 6 * B)], UP2, up)
    down2 = remote(halo.at[3, :, :, pl.ds(0, 6 * B)], halo.at[4, :, :, pl.ds(0, 6 * B)], DOWN2, down)
    pair_cols = ((3, 6), (1, 8), (0, 8), (0, 6))
    pair_copies = []
    for q in range(4):
        cols = pl.ds(pair_cols[q][0] * B, pair_cols[q][1] * B)
        pair_copies.append(
            remote(
                halo.at[q + 1 - core, :, :, cols], pair_halo.at[q, :, :, cols], PAIR + q, mate
            )
        )

    gram[...] = jnp.zeros_like(gram)
    terms[...] = jnp.zeros_like(terms)
    x_buf[...] = jnp.zeros_like(x_buf)
    v_buf[...] = jnp.zeros_like(v_buf)

    widths = []
    for t in range(SLOTS):
        block = ci + t - 4
        inside = (block >= 0) & (block < nchain)
        width = profile_ref[jnp.clip(block, 0, nchain - 1)]
        widths.append(jnp.where(inside, width, -1))
    row_ok = [jnp.abs(k - 4) <= jnp.minimum(widths[4], widths[k]) for k in range(SLOTS)]
    keep = [jnp.where(ok, 1.0, 0.0).astype(F32) for ok in row_ok]

    def assemble(d):
        k = d + 4
        for which, target in ((0, x_buf), (1, v_buf)):
            for c in range(max(0, d), min(8, 8 + d) + 1):
                ok = row_ok[k] & (abs(c - k) <= jnp.minimum(widths[k], widths[c]))
                factor = jnp.where(ok, 1.0, 0.0).astype(F32)
                cols = pl.ds((c - d) * B, B)
                if d % 2 == 0:
                    block = halo[2 + d // 2, which, :, cols]
                else:
                    block = pair_halo[(d + 3) // 2, which, :, cols]
                block = (block.astype(F32) * factor).astype(BF16)
                if c == 8:
                    xv_last[pl.ds((k - 4) * B, B), pl.ds(which * B, B)] = block
                else:
                    target[pl.ds(k * B, B), pl.ds(c * B, B)] = block

    assemble(0)
    up1.wait_recv()
    up2.start()
    down1.wait_recv()
    down2.start()
    pair_copies[1].start()
    pair_copies[2].start()

    @pl.when(core == 0)
    def _():
        pair_copies[0].start()

    @pl.when(core == 1)
    def _():
        pair_copies[3].start()

    assemble(-2)
    assemble(2)

    info_copy.wait_recv()
    tall = naux * ROWS
    lane = lax.broadcasted_iota(jnp.int32, (tall, B), 1)
    tall_row = lax.broadcasted_iota(jnp.int32, (tall, B), 0)
    pick = jnp.where(lax.div(tall_row, ROWS) == lane, 1.0, 0.0).astype(F32)
    kern_all = info[:, 0].reshape(naux, B)
    screen_all = info[:, 1].reshape(naux, B)
    screen_tall = jnp.broadcast_to(screen_all[:, None, :], (naux, ROWS, B)).reshape(tall, B)
    kern_tall = jnp.broadcast_to((kern_all * screen_all)[:, None, :], (naux, ROWS, B)).reshape(tall, B)
    spread = lax.dot_general(
        kern_tall.astype(BF16),
        (pick * screen_tall).astype(BF16),
        (((1,), (1,)), ((), ())),
        preferred_element_type=F32,
    )
    same_row = lax.rem(lax.broadcasted_iota(jnp.int32, (tall, tall), 0), ROWS) == lax.rem(
        lax.broadcasted_iota(jnp.int32, (tall, tall), 1), ROWS
    )
    kron[...] = jnp.where(same_row, spread, 0.0).astype(BF16)

    up2.wait_recv()
    down2.wait_recv()

    @pl.when(core == 1)
    def _():
        pair_copies[0].start()

    @pl.when(core == 0)
    def _():
        pair_copies[3].start()

    assemble(-4)
    assemble(4)
    for q, d in ((1, -1), (2, 1), (0, -3), (3, 3)):
        pair_copies[q].wait_recv()
        assemble(d)

    def arrived(g):
        pltpu.make_async_copy(
            tc_hbm.at[:, chunks * a + g], s_buf.at[g, pl.ds(half * a, half)], local_sem.at[2 + g]
        ).wait()
        remote(
            tc_hbm.at[:, chunks * (1 - a) + g],
            s_buf.at[g, pl.ds(half * (1 - a), half)],
            S_IN + g,
            twin,
        ).wait_recv()

    def step(g, carry):
        arrived(g)

        def cut(k0, k1):
            return s_buf[g, :, :, pl.ds(k0 * B, (k1 - k0) * B)].reshape(tall, (k1 - k0) * B)

        for c0, c1, k0, k1 in TILES:
            cols = pl.ds(c0 * B, (c1 - c0) * B)
            rows = pl.ds(k0 * B, (k1 - k0) * B)
            coupled[:, cols] = jnp.dot(cut(k0, k1), x_buf[rows, cols], preferred_element_type=F32).astype(BF16)
            partner[:, cols] = jnp.dot(cut(k0, k1), v_buf[rows, cols], preferred_element_type=F32).astype(BF16)
        last = jnp.dot(cut(4, 9), xv_last[...], preferred_element_type=F32).astype(BF16)
        coupled[:, pl.ds(8 * B, B)] = last[:, :B]
        partner[:, pl.ds(8 * B, B)] = last[:, B:]
        gram[...] += lax.dot_general(
            coupled[...], partner[...], (((1,), (1,)), ((), ())), preferred_element_type=F32
        )
        response[...] = jnp.dot(kron[...], partner[...], preferred_element_type=F32).astype(BF16)
        s_t[...] = cut(0, 9).T
        for c0, c1, k0, k1 in TILES + ((8, 9, 4, 9),):
            cols = pl.ds(c0 * B, (c1 - c0) * B)
            rows = pl.ds(k0 * B, (k1 - k0) * B)
            terms[rows, cols] += jnp.dot(s_t[rows, :], response[:, cols], preferred_element_type=F32)
        return carry

    lax.fori_loop(0, chunks, step, 0)

    def own_terms(d, cj0, cj1):
        k = d + 4
        return terms[pl.ds(k * B, B), pl.ds((cj0 + d) * B, (cj1 - cj0) * B)] * keep[k]

    gpair = []
    for q, d in enumerate((-3, -1, 1, 3)):
        c0, n = pair_cols[q]
        cols = pl.ds(c0 * B, n * B)
        pair_out[q, :, cols] = own_terms(d, c0, c0 + n).astype(BF16)
        copy = remote(pair_out.at[q, :, cols], pair_in.at[q + core, :, cols], GPAIR + q, mate)
        copy.start()
        gpair.append(copy)

    folded = jnp.where(same_row, gram[...], 0.0).reshape(naux, ROWS, tall).sum(1)
    polar = jnp.dot(folded, pick, preferred_element_type=F32, precision=lax.Precision.HIGHEST)
    square_row = lax.broadcasted_iota(jnp.int32, (naux, B), 0)
    square_lane = lax.broadcasted_iota(jnp.int32, (naux, B), 1)
    screen_lane = jnp.sum(jnp.where(square_row == square_lane, screen_all, 0.0), axis=0, keepdims=True)
    polar = polar * screen_all * screen_lane
    pol_out[0] = polar
    pol_copies = [
        remote(pol_out.at[r], pol_in.at[r], POLAR + r, polar_peers[r]) for r in range(rounds)
    ]
    pol_copies[0].start()

    def polar_round(r):
        pol_copies[r].wait_recv()
        pol_out[r + 1] = pol_out[r] + pol_in[r]
        if r + 1 < rounds:
            pol_copies[r + 1].start()

    for copy in gpair:
        copy.wait_recv()
    out2[0] = jnp.concatenate(
        [
            own_terms(4, 0, 5) + pair_in[4, :, pl.ds(0, 5 * B)].astype(F32),
            pair_in[4, :, pl.ds(5 * B, B)].astype(F32),
        ],
        axis=1,
    ).astype(BF16)
    gup2 = remote(out2.at[0], in2.at[0], GUP2, up)
    gup2.start()
    out2[1] = jnp.concatenate(
        [
            pair_in[0, :, pl.ds(3 * B, B)].astype(F32),
            own_terms(-4, 4, 9) + pair_in[0, :, pl.ds(4 * B, 5 * B)].astype(F32),
        ],
        axis=1,
    ).astype(BF16)
    gdown2 = remote(out2.at[1], in2.at[1], GDOWN2, down)
    gdown2.start()
    polar_round(0)
    polar_round(1)

    gup2.wait_recv()
    for c in range(8):
        cols = pl.ds(c * B, B)
        part = pair_in[3, :, cols].astype(F32)
        if c < 7:
            part = part + own_terms(2, c, c + 1)
        if c < 6:
            part = part + in2[0, :, cols].astype(F32)
        out1[0, :, cols] = part.astype(BF16)
    gup1 = remote(out1.at[0], in1.at[0], GUP1, up)
    gup1.start()
    gdown2.wait_recv()
    for c in range(8):
        cols = pl.ds(c * B, B)
        part = pair_in[1, :, pl.ds((c + 1) * B, B)].astype(F32)
        if c >= 1:
            part = part + own_terms(-2, c + 1, c + 2)
        if c >= 2:
            part = part + in2[1, :, pl.ds((c - 2) * B, B)].astype(F32)
        out1[1, :, cols] = part.astype(BF16)
    gdown1 = remote(out1.at[1], in1.at[1], GDOWN1, down)
    gdown1.start()
    for r in range(2, rounds):
        polar_round(r)
    pol_ref[...] = pol_out[rounds, pl.ds(half * a, half), pl.ds(0, naux)] * scale_pol

    total[...] = terms[pl.ds(4 * B, B), :] + pair_in[2].astype(F32)
    gup1.wait_recv()
    total[:, pl.ds(0, 8 * B)] += in1[0].astype(F32)
    gdown1.wait_recv()
    total[:, pl.ds(B, 8 * B)] += in1[1].astype(F32)
    rows = B // 2
    aux_out[...] = total[pl.ds(rows * (1 - a), rows), :].astype(BF16)
    gaux = remote(aux_out, aux_in, GAUX, twin)
    gaux.start()
    gaux.wait_recv()
    for c in range(SLOTS):
        cols = pl.ds(c * B, B)
        grad_ref[:, cols] = (
            total[pl.ds(rows * a, rows), cols] + aux_in[:, cols].astype(F32)
        ) * (keep[c] * scale_grad)

    info_copy.wait_send()
    for g in range(chunks):
        remote(
            tc_hbm.at[:, chunks * (1 - a) + g],
            s_buf.at[g, pl.ds(half * a, half)],
            S_IN + g,
            twin,
        ).wait_send()
    for copy in [up1, down1, up2, down2] + pair_copies + gpair + [gup2, gdown2, gup1, gdown1, gaux] + pol_copies:
        copy.wait_send()


def body(occupied, virtual, three_centre, kern, profile, atom_map):
    nchain = lax.axis_size("chain")
    half = three_centre.shape[0]
    naux = kern.shape[1]
    chunks = (B // 2) // ROWS
    tall = naux * ROWS
    rounds = int(math.log2(nchain)) + 1
    slabs = three_centre.reshape(half, B // ROWS, ROWS, W)
    anyspace = pl.BlockSpec(memory_space=pl.ANY)
    vmem = pl.BlockSpec(memory_space=pltpu.VMEM)
    smem = pl.BlockSpec(memory_space=pltpu.SMEM)
    grad, pol = pl.pallas_call(
        functools.partial(
            kernel,
            nchain,
            naux,
            nchain // 4,
            1.0 / math.sqrt(B * naux),
            1.0 / math.sqrt(B * nchain * W),
        ),
        out_shape=(
            jax.ShapeDtypeStruct((B // 2, W), F32),
            jax.ShapeDtypeStruct((half, naux), F32),
        ),
        in_specs=[anyspace, anyspace, anyspace, vmem, smem, smem],
        out_specs=(vmem, vmem),
        scratch_shapes=[
            pltpu.VMEM((chunks, naux, ROWS, W), BF16),
            pltpu.VMEM((5, 2, B, W), BF16),
            pltpu.VMEM((4, 2, B, W), BF16),
            pltpu.VMEM((W, W), BF16),
            pltpu.VMEM((W, W), BF16),
            pltpu.VMEM((5 * B, 2 * B), BF16),
            pltpu.VMEM((W, tall), BF16),
            pltpu.VMEM((tall, W), BF16),
            pltpu.VMEM((tall, W), BF16),
            pltpu.VMEM((tall, W), BF16),
            pltpu.VMEM((tall, tall), F32),
            pltpu.VMEM((tall, tall), BF16),
            pltpu.VMEM((2, 2, half, B), F32),
            pltpu.VMEM((W, W), F32),
            pltpu.VMEM((4, B, W), BF16),
            pltpu.VMEM((5, B, W), BF16),
            pltpu.VMEM((2, B, 6 * B), BF16),
            pltpu.VMEM((2, B, 6 * B), BF16),
            pltpu.VMEM((2, B, 8 * B), BF16),
            pltpu.VMEM((2, B, 8 * B), BF16),
            pltpu.VMEM((B, W), F32),
            pltpu.VMEM((B // 2, W), BF16),
            pltpu.VMEM((B // 2, W), BF16),
            pltpu.VMEM((rounds + 1, naux, B), F32),
            pltpu.VMEM((rounds, naux, B), F32),
            pltpu.SemaphoreType.DMA((POLAR + rounds,)),
            pltpu.SemaphoreType.DMA((POLAR + rounds,)),
            pltpu.SemaphoreType.DMA((2 + chunks,)),
        ],
        compiler_params=pltpu.CompilerParams(
            collective_id=0, has_side_effects=True, vmem_limit_bytes=60 * 2**20
        ),
        name="rpa",
    )(occupied, virtual, slabs, kern, profile, atom_map)
    return grad, pol


def solution(mesh):
    placed = (
        P("chain", None),
        P("chain", None),
        P("aux", "chain", None),
        P("aux", None),
        P(),
        P("aux"),
    )
    return jax.shard_map(
        body,
        mesh=mesh,
        in_specs=placed,
        out_specs=(P(("chain", "aux"), None), P("aux", None)),
        check_vma=False,
    )
```

```python
import functools
import math

import jax
import jax.numpy as jnp
from jax import lax
from jax.experimental import pallas as pl
from jax.experimental.pallas import tpu as pltpu
from jax.sharding import PartitionSpec as P

MESH = pl.DeviceIdType.MESH
BF16 = jnp.bfloat16
F32 = jnp.float32
B = 128
SLOTS = 9
W = SLOTS * B
ROWS = 16
TILES = ((0, 2, 0, 6), (2, 4, 0, 8), (4, 6, 0, 9), (6, 8, 2, 9))

S_IN = 0
UP1, DOWN1, UP2, DOWN2 = 4, 5, 6, 7
PAIR = 8
INFO = 12
GPAIR = 13
GUP2, GDOWN2, GUP1, GDOWN1, GAUX = 21, 23, 25, 27, 29
POLAR = 31
PIECES = 2
RUN = B // 4
VMEM_LIMIT = 60 * 2**20


def kernel(
    nchain,
    naux,
    reach,
    scale_grad,
    scale_pol,
    occ_hbm,
    vir_hbm,
    tc_hbm,
    kern_hbm,
    profile_hbm,
    atom_hbm,
    grad_ref,
    pol_ref,
    s_buf,
    halo,
    pair_halo,
    x_buf,
    v_buf,
    xv_last,
    s_t,
    coupled,
    partner,
    response,
    gram,
    kron,
    info,
    terms,
    pair_out,
    pair_in,
    out2,
    in2,
    out1,
    in1,
    total,
    aux_out,
    aux_in,
    pol_out,
    pol_in,
    kern_ref,
    profile_ref,
    atom_ref,
    send_sem,
    recv_sem,
    local_sem,
):
    half = naux // 2
    chunks = (B // 2) // ROWS
    chips = nchain // 2
    ci = lax.axis_index("chain")
    a = lax.axis_index("aux")
    chip = lax.div(ci, 2)
    core = lax.rem(ci, 2)
    inrow = lax.rem(chip, 4)
    flip_up = lax.div(inrow + 1, 4)
    flip_down = 1 - lax.div(inrow + 3, 4)
    up = (2 * lax.rem(chip + 1, chips) + core, lax.rem(a + flip_up, 2))
    down = (2 * lax.rem(chip + chips - 1, chips) + core, lax.rem(a + flip_down, 2))
    mate = (2 * chip + 1 - core, a)
    twin = (ci, 1 - a)

    def across(bit):
        size = 1 << bit
        return (ci + size * (1 - 2 * lax.rem(lax.div(ci, size), 2)), a)

    def xor(low, value):
        device = ci
        for bit in (0, 1):
            if value >> bit & 1:
                size = 1 << (low + bit)
                device = device + size * (1 - 2 * lax.rem(lax.div(ci, size), 2))
        return (device, a)

    groups = [[mate], [twin]]
    if nchain >= 64:
        groups.append([xor(4, v) for v in (1, 2, 3)])
    if nchain >= 16:
        groups.append([xor(3, 1)])
    groups.append([xor(1, v) for v in (1, 2, 3)])
    polar_peers = [device for group in groups for device in group]

    def remote(src, dst, number, device):
        return pltpu.make_async_remote_copy(
            src_ref=src,
            dst_ref=dst,
            send_sem=send_sem.at[number],
            recv_sem=recv_sem.at[number],
            device_id=device,
            device_id_type=MESH,
        )

    own_copies = [
        pltpu.make_async_copy(occ_hbm, halo.at[2, 0], local_sem.at[0]),
        pltpu.make_async_copy(vir_hbm, halo.at[2, 1], local_sem.at[1]),
    ]
    slab_copies = [
        pltpu.make_async_copy(
            tc_hbm.at[:, chunks * a + g], s_buf.at[g, pl.ds(half * a, half)], local_sem.at[2 + g]
        )
        for g in range(chunks)
    ]
    table_copies = [
        pltpu.make_async_copy(src, dst, local_sem.at[2 + chunks + n])
        for n, (src, dst) in enumerate(
            ((kern_hbm, kern_ref), (profile_hbm, profile_ref), (atom_hbm, atom_ref))
        )
    ]

    for slot, c0, n in ((0, 3, 6), (1, 1, 2), (2, 0, 1), (2, 8, 1), (3, 6, 2), (4, 0, 6)):
        pair_in[slot, :, pl.ds(c0 * B, n * B)] = jnp.zeros((B, n * B), BF16)

    barrier = pltpu.get_barrier_semaphore()
    greeted = [up, down] + polar_peers
    for device in greeted:
        pl.semaphore_signal(barrier, inc=1, device_id=device, device_id_type=MESH)
    for copy in own_copies + table_copies + slab_copies:
        copy.start()
    for copy in table_copies:
        copy.wait()
    row_id = lax.broadcasted_iota(jnp.int32, (half, B), 0)
    screen = jnp.zeros((half, B), F32)
    for p in range(half):
        near = jnp.abs(atom_ref[p] - ci) <= reach
        screen = jnp.where(row_id == p, jnp.where(near, 1.0, 0.0).astype(F32), screen)
    info[a, 0] = jnp.zeros((half, B), F32)
    info[a, 0, :, pl.ds(0, naux)] = kern_ref[...].astype(F32)
    info[a, 1] = screen
    pl.semaphore_wait(barrier, len(greeted))

    info_copy = remote(info.at[a], info.at[a], INFO, twin)
    for g in range(chunks):
        remote(
            tc_hbm.at[:, chunks * (1 - a) + g],
            s_buf.at[g, pl.ds(half * a, half)],
            S_IN + g,
            twin,
        ).start()
        if g == 0:
            info_copy.start()
    for copy in own_copies:
        copy.wait()
    up1 = remote(halo.at[2, :, :, pl.ds(B, 8 * B)], halo.at[1, :, :, pl.ds(B, 8 * B)], UP1, up)
    down1 = remote(halo.at[2, :, :, pl.ds(0, 8 * B)], halo.at[3, :, :, pl.ds(0, 8 * B)], DOWN1, down)
    up1.start()
    down1.start()
    up2 = remote(halo.at[1, :, :, pl.ds(3 * B, 6 * B)], halo.at[0, :, :, pl.ds(3 * B, 6 * B)], UP2, up)
    down2 = remote(halo.at[3, :, :, pl.ds(0, 6 * B)], halo.at[4, :, :, pl.ds(0, 6 * B)], DOWN2, down)
    pair_cols = ((3, 6), (1, 8), (0, 8), (0, 6))
    pair_copies = []
    for q in range(4):
        cols = pl.ds(pair_cols[q][0] * B, pair_cols[q][1] * B)
        pair_copies.append(
            remote(
                halo.at[q + 1 - core, :, :, cols], pair_halo.at[q, :, :, cols], PAIR + q, mate
            )
        )

    gram[...] = jnp.zeros_like(gram)
    coupled[...] = jnp.zeros_like(coupled)
    partner[...] = jnp.zeros_like(partner)
    terms[...] = jnp.zeros_like(terms)
    x_buf[...] = jnp.zeros_like(x_buf)
    v_buf[...] = jnp.zeros_like(v_buf)

    widths = []
    for t in range(SLOTS):
        block = ci + t - 4
        inside = (block >= 0) & (block < nchain)
        width = profile_ref[jnp.clip(block, 0, nchain - 1)]
        widths.append(jnp.where(inside, width, -1))
    row_ok = [jnp.abs(k - 4) <= jnp.minimum(widths[4], widths[k]) for k in range(SLOTS)]
    keep = [jnp.where(ok, 1.0, 0.0).astype(F32) for ok in row_ok]

    def assemble(d):
        k = d + 4
        for which, target in ((0, x_buf), (1, v_buf)):
            for c in range(max(0, d), min(8, 8 + d) + 1):
                ok = row_ok[k] & (abs(c - k) <= jnp.minimum(widths[k], widths[c]))
                factor = jnp.where(ok, 1.0, 0.0).astype(F32)
                cols = pl.ds((c - d) * B, B)
                if d % 2 == 0:
                    block = halo[2 + d // 2, which, :, cols]
                else:
                    block = pair_halo[(d + 3) // 2, which, :, cols]
                block = (block.astype(F32) * factor).astype(BF16)
                if c == 8:
                    xv_last[pl.ds((k - 4) * B, B), pl.ds(which * B, B)] = block
                else:
                    target[pl.ds(k * B, B), pl.ds(c * B, B)] = block

    assemble(0)
    up1.wait_recv()
    up2.start()
    down1.wait_recv()
    down2.start()
    pair_copies[1].start()
    pair_copies[2].start()

    @pl.when(core == 0)
    def _():
        pair_copies[0].start()

    @pl.when(core == 1)
    def _():
        pair_copies[3].start()

    assemble(-2)
    assemble(2)

    info_copy.wait_recv()
    tall = naux * ROWS
    lane = lax.broadcasted_iota(jnp.int32, (tall, B), 1)
    tall_row = lax.broadcasted_iota(jnp.int32, (tall, B), 0)
    pick = jnp.where(lax.div(tall_row, ROWS) == lane, 1.0, 0.0).astype(F32)
    kern_all = info[:, 0].reshape(naux, B)
    screen_all = info[:, 1].reshape(naux, B)
    screen_tall = jnp.broadcast_to(screen_all[:, None, :], (naux, ROWS, B)).reshape(tall, B)
    kern_tall = jnp.broadcast_to((kern_all * screen_all)[:, None, :], (naux, ROWS, B)).reshape(tall, B)
    spread = lax.dot_general(
        kern_tall.astype(BF16),
        (pick * screen_tall).astype(BF16),
        (((1,), (1,)), ((), ())),
        preferred_element_type=F32,
    )
    same_row = lax.rem(lax.broadcasted_iota(jnp.int32, (tall, tall), 0), ROWS) == lax.rem(
        lax.broadcasted_iota(jnp.int32, (tall, tall), 1), ROWS
    )
    kron[...] = jnp.where(same_row, spread, 0.0).astype(BF16)

    up2.wait_recv()
    down2.wait_recv()

    @pl.when(core == 1)
    def _():
        pair_copies[0].start()

    @pl.when(core == 0)
    def _():
        pair_copies[3].start()

    assemble(-4)
    assemble(4)
    for q, d in ((1, -1), (2, 1), (0, -3), (3, 3)):
        pair_copies[q].wait_recv()
        assemble(d)

    def add_gram():
        gram[...] += lax.dot_general(
            coupled[...], partner[...], (((1,), (1,)), ((), ())), preferred_element_type=F32
        )

    def products(g, slab):
        mine = pl.ds(half * slab, half)
        short = half * ROWS
        tall_rows = pl.ds(pl.multiple_of(short * slab, short), short)

        def cut(k0, k1):
            return s_buf[g, mine, :, pl.ds(k0 * B, (k1 - k0) * B)].reshape(short, (k1 - k0) * B)

        for c0, c1, k0, k1 in TILES:
            cols = pl.ds(c0 * B, (c1 - c0) * B)
            rows = pl.ds(k0 * B, (k1 - k0) * B)
            coupled[tall_rows, cols] = jnp.dot(cut(k0, k1), x_buf[rows, cols], preferred_element_type=F32).astype(BF16)
            partner[tall_rows, cols] = jnp.dot(cut(k0, k1), v_buf[rows, cols], preferred_element_type=F32).astype(BF16)
        last = jnp.dot(cut(4, 9), xv_last[...], preferred_element_type=F32).astype(BF16)
        coupled[tall_rows, pl.ds(8 * B, B)] = last[:, :B]
        partner[tall_rows, pl.ds(8 * B, B)] = last[:, B:]

    def step(g, carry):
        pltpu.make_async_copy(
            tc_hbm.at[:, chunks * a + g], s_buf.at[g, pl.ds(half * a, half)], local_sem.at[2 + g]
        ).wait()
        products(g, a)
        remote(
            tc_hbm.at[:, chunks * (1 - a) + g],
            s_buf.at[g, pl.ds(half * (1 - a), half)],
            S_IN + g,
            twin,
        ).wait_recv()
        products(g, 1 - a)
        add_gram()
        response[...] = jnp.dot(kron[...], partner[...], preferred_element_type=F32).astype(BF16)
        s_t[...] = s_buf[g].reshape(tall, W).T
        for c0, c1, k0, k1 in TILES + ((8, 9, 4, 9),):
            cols = pl.ds(c0 * B, (c1 - c0) * B)
            rows = pl.ds(k0 * B, (k1 - k0) * B)
            terms[rows, cols] += jnp.dot(s_t[rows, :], response[:, cols], preferred_element_type=F32)
        return carry

    lax.fori_loop(0, chunks, step, 0)

    def own_terms(p, run, d, cj, n=1):
        k = d + 4
        return terms[pl.ds(k * B + run * 2 * RUN + p * RUN, RUN), pl.ds((cj + d) * B, n * B)] * keep[k]

    def mates(p, run, slot, cj):
        return pair_in[slot, pl.ds((2 * p + run) * RUN, RUN), pl.ds(cj * B, B)].astype(F32)

    def piece(p):
        return pl.ds(2 * p * RUN, 2 * RUN)

    gpair = [[None] * 4 for _ in range(PIECES)]
    for p in range(PIECES):
        for q in (0, 3, 1, 2):
            c0, n = pair_cols[q]
            cols = pl.ds(c0 * B, n * B)
            for run in (0, 1):
                pair_out[q, pl.ds((2 * p + run) * RUN, RUN), cols] = own_terms(p, run, 2 * q - 3, c0, n).astype(BF16)
            gpair[p][q] = remote(
                pair_out.at[q, piece(p), cols],
                pair_in.at[q + core, piece(p), cols],
                GPAIR + 4 * p + q,
                mate,
            )
            gpair[p][q].start()

    gup2, gdown2, gup1, gdown1, gaux = [], [], [], [], []
    for p in range(PIECES):
        for q in (0, 3, 1, 2):
            gpair[p][q].wait_recv()
        for run in (0, 1):
            at = pl.ds((2 * p + run) * RUN, RUN)
            for c in range(6):
                part = mates(p, run, 4, c)
                if c < 5:
                    part = part + own_terms(p, run, 4, c)
                out2[0, at, pl.ds(c * B, B)] = part.astype(BF16)
        gup2.append(remote(out2.at[0, piece(p)], in2.at[0, piece(p)], GUP2 + p, up))
        gup2[p].start()
        for run in (0, 1):
            at = pl.ds((2 * p + run) * RUN, RUN)
            for c in range(6):
                part = mates(p, run, 0, c + 3)
                if c >= 1:
                    part = part + own_terms(p, run, -4, c + 3)
                out2[1, at, pl.ds(c * B, B)] = part.astype(BF16)
        gdown2.append(remote(out2.at[1, piece(p)], in2.at[1, piece(p)], GDOWN2 + p, down))
        gdown2[p].start()

    folded = jnp.where(same_row, gram[...], 0.0).reshape(naux, ROWS, tall).sum(1)
    polar = jnp.dot(folded, pick, preferred_element_type=F32, precision=lax.Precision.HIGHEST)
    square_row = lax.broadcasted_iota(jnp.int32, (naux, B), 0)
    square_lane = lax.broadcasted_iota(jnp.int32, (naux, B), 1)
    screen_lane = jnp.sum(jnp.where(square_row == square_lane, screen_all, 0.0), axis=0, keepdims=True)
    pol_out[0] = polar * screen_all * screen_lane
    pol_copies = []
    for r, group in enumerate(groups):
        first = sum(len(g) for g in groups[:r])
        pol_copies.append(
            [
                remote(pol_out.at[r], pol_in.at[first + n], POLAR + first + n, device)
                for n, device in enumerate(group)
            ]
        )

    def polar_start(r):
        for copy in pol_copies[r]:
            copy.start()

    def polar_round(r):
        for copy in pol_copies[r]:
            copy.wait_recv()
        first = sum(len(g) for g in groups[:r])
        value = pol_out[r] + pol_in[first]
        if len(groups[r]) == 3:
            value = value + (pol_in[first + 1] + pol_in[first + 2])
        pol_out[r + 1] = value
        if r + 1 < len(groups):
            polar_start(r + 1)

    polar_start(0)
    polar_round(0)
    for p in range(PIECES):
        gup2[p].wait_recv()
        for run in (0, 1):
            at = pl.ds((2 * p + run) * RUN, RUN)
            for c in range(8):
                part = mates(p, run, 3, c)
                if c < 7:
                    part = part + own_terms(p, run, 2, c)
                if c < 6:
                    part = part + in2[0, at, pl.ds(c * B, B)].astype(F32)
                out1[0, at, pl.ds(c * B, B)] = part.astype(BF16)
        gup1.append(remote(out1.at[0, piece(p)], in1.at[0, piece(p)], GUP1 + p, up))
        gup1[p].start()
        gdown2[p].wait_recv()
        for run in (0, 1):
            at = pl.ds((2 * p + run) * RUN, RUN)
            for c in range(8):
                part = mates(p, run, 1, c + 1)
                if c >= 1:
                    part = part + own_terms(p, run, -2, c + 1)
                if c >= 2:
                    part = part + in2[1, at, pl.ds((c - 2) * B, B)].astype(F32)
                out1[1, at, pl.ds(c * B, B)] = part.astype(BF16)
        gdown1.append(remote(out1.at[1, piece(p)], in1.at[1, piece(p)], GDOWN1 + p, down))
        gdown1[p].start()
        if p + 1 < len(groups) - 1:
            polar_round(p + 1)
    for p in range(PIECES):
        gup1[p].wait_recv()
        gdown1[p].wait_recv()
        for run in (0, 1):
            at = pl.ds((2 * p + run) * RUN, RUN)
            for c in range(SLOTS):
                part = mates(p, run, 2, c) + own_terms(p, run, 0, c)
                if c < 8:
                    part = part + in1[0, at, pl.ds(c * B, B)].astype(F32)
                if c >= 1:
                    part = part + in1[1, at, pl.ds((c - 1) * B, B)].astype(F32)
                total[run, pl.ds(p * RUN, RUN), pl.ds(c * B, B)] = part
        there = pl.ds(p * RUN, RUN)
        aux_out[there, :] = total[1 - a, there, :].astype(BF16)
        gaux.append(remote(aux_out.at[there], aux_in.at[there], GAUX + p, twin))
        gaux[p].start()
        if p + PIECES + 1 < len(groups) - 1:
            polar_round(p + PIECES + 1)
    for r in range(min(2 * PIECES + 1, len(groups) - 1), len(groups) - 1):
        polar_round(r)
    for p in range(PIECES):
        gaux[p].wait_recv()
        there = pl.ds(p * RUN, RUN)
        for c in range(SLOTS):
            cols = pl.ds(c * B, B)
            grad_ref[there, cols] = (
                total[a, there, cols] + aux_in[there, cols].astype(F32)
            ) * (keep[c] * scale_grad)
    polar_round(len(groups) - 1)
    pol_ref[...] = pol_out[len(groups), pl.ds(half * a, half), pl.ds(0, naux)] * scale_pol

    info_copy.wait_send()
    for g in range(chunks):
        remote(
            tc_hbm.at[:, chunks * (1 - a) + g],
            s_buf.at[g, pl.ds(half * a, half)],
            S_IN + g,
            twin,
        ).wait_send()
    sent = [up1, down1, up2, down2] + pair_copies + gup2 + gdown2 + gup1 + gdown1 + gaux
    for copy in sent + [copy for group in gpair + pol_copies for copy in group]:
        copy.wait_send()


def body(occupied, virtual, three_centre, kern, profile, atom_map):
    nchain = lax.axis_size("chain")
    half = three_centre.shape[0]
    naux = kern.shape[1]
    chunks = (B // 2) // ROWS
    tall = naux * ROWS
    polars = 5 + 3 * (nchain >= 64) + (nchain >= 16)
    rounds = 3 + (nchain >= 64) + (nchain >= 16)
    slabs = three_centre.reshape(half, B // ROWS, ROWS, W)
    hbm = pl.BlockSpec(memory_space=pltpu.HBM)
    vmem = pl.BlockSpec(memory_space=pltpu.VMEM)
    grad, pol = pl.pallas_call(
        functools.partial(
            kernel,
            nchain,
            naux,
            nchain // 4,
            1.0 / math.sqrt(B * naux),
            1.0 / math.sqrt(B * nchain * W),
        ),
        out_shape=(
            jax.ShapeDtypeStruct((B // 2, W), F32),
            jax.ShapeDtypeStruct((half, naux), F32),
        ),
        in_specs=[hbm] * 6,
        out_specs=(vmem, vmem),
        scratch_shapes=[
            pltpu.VMEM((chunks, naux, ROWS, W), BF16),
            pltpu.VMEM((5, 2, B, W), BF16),
            pltpu.VMEM((4, 2, B, W), BF16),
            pltpu.VMEM((W, W), BF16),
            pltpu.VMEM((W, W), BF16),
            pltpu.VMEM((5 * B, 2 * B), BF16),
            pltpu.VMEM((W, tall), BF16),
            pltpu.VMEM((tall, W), BF16),
            pltpu.VMEM((tall, W), BF16),
            pltpu.VMEM((tall, W), BF16),
            pltpu.VMEM((tall, tall), F32),
            pltpu.VMEM((tall, tall), BF16),
            pltpu.VMEM((2, 2, half, B), F32),
            pltpu.VMEM((W, W), F32),
            pltpu.VMEM((4, B, W), BF16),
            pltpu.VMEM((5, B, W), BF16),
            pltpu.VMEM((2, B, 6 * B), BF16),
            pltpu.VMEM((2, B, 6 * B), BF16),
            pltpu.VMEM((2, B, 8 * B), BF16),
            pltpu.VMEM((2, B, 8 * B), BF16),
            pltpu.VMEM((2, B // 2, W), F32),
            pltpu.VMEM((B // 2, W), BF16),
            pltpu.VMEM((B // 2, W), BF16),
            pltpu.VMEM((rounds + 1, naux, B), F32),
            pltpu.VMEM((polars, naux, B), F32),
            pltpu.VMEM((half, naux), BF16),
            pltpu.SMEM((nchain,), jnp.int32),
            pltpu.SMEM((half,), jnp.int32),
            pltpu.SemaphoreType.DMA((POLAR + polars,)),
            pltpu.SemaphoreType.DMA((POLAR + polars,)),
            pltpu.SemaphoreType.DMA((5 + chunks,)),
        ],
        compiler_params=pltpu.CompilerParams(
            collective_id=0, has_side_effects=True, vmem_limit_bytes=VMEM_LIMIT
        ),
        name="rpa",
    )(occupied, virtual, slabs, kern, profile, atom_map)
    return grad, pol


def solution(mesh):
    placed = (
        P("chain", None),
        P("chain", None),
        P("aux", "chain", None),
        P("aux", None),
        P(),
        P("aux"),
    )
    return jax.shard_map(
        body,
        mesh=mesh,
        in_specs=placed,
        out_specs=(P(("chain", "aux"), None), P("aux", None)),
        check_vma=False,
    )
```

```python
import functools
import math

import jax
import jax.numpy as jnp
from jax import lax
from jax.experimental import pallas as pl
from jax.experimental.pallas import tpu as pltpu
from jax.sharding import PartitionSpec as P

MESH = pl.DeviceIdType.MESH
BF16 = jnp.bfloat16
F32 = jnp.float32
B = 128
SLOTS = 9
W = SLOTS * B
ROWS = 16
TILES = ((0, 2, 0, 6), (2, 4, 0, 8), (4, 6, 0, 9), (6, 8, 2, 9))

S_IN = 0
UP1, DOWN1, UP2, DOWN2 = 4, 5, 6, 7
PAIR = 8
INFO = 12
GPAIR = 13
PIECES = 2
RUN = B // (2 * PIECES)
GUP2, GDOWN2, GUP1, GDOWN1, GAUX, POLAR = [GPAIR + n * PIECES for n in (4, 5, 6, 7, 8, 9)]
VMEM_LIMIT = 44 * 2**20


def kernel(
    nchain,
    naux,
    reach,
    scale_grad,
    scale_pol,
    occ_hbm,
    vir_hbm,
    tc_hbm,
    kern_hbm,
    profile_hbm,
    atom_hbm,
    grad_ref,
    pol_ref,
    s_buf,
    halo,
    pair_halo,
    x_buf,
    v_buf,
    xv_last,
    s_t,
    coupled,
    partner,
    response,
    gram,
    kron,
    info,
    terms,
    pair_out,
    pair_in,
    out2,
    in2,
    out1,
    in1,
    total,
    aux_out,
    aux_in,
    pol_out,
    pol_in,
    kern_ref,
    profile_ref,
    atom_ref,
    send_sem,
    recv_sem,
    local_sem,
):
    half = naux // 2
    chunks = (B // 2) // ROWS
    chips = nchain // 2
    ci = lax.axis_index("chain")
    a = lax.axis_index("aux")
    chip = lax.div(ci, 2)
    core = lax.rem(ci, 2)
    inrow = lax.rem(chip, 4)
    flip_up = lax.div(inrow + 1, 4)
    flip_down = 1 - lax.div(inrow + 3, 4)
    up = (2 * lax.rem(chip + 1, chips) + core, lax.rem(a + flip_up, 2))
    down = (2 * lax.rem(chip + chips - 1, chips) + core, lax.rem(a + flip_down, 2))
    mate = (2 * chip + 1 - core, a)
    twin = (ci, 1 - a)

    def across(bit):
        size = 1 << bit
        return (ci + size * (1 - 2 * lax.rem(lax.div(ci, size), 2)), a)

    def xor(low, value):
        device = ci
        for bit in (0, 1):
            if value >> bit & 1:
                size = 1 << (low + bit)
                device = device + size * (1 - 2 * lax.rem(lax.div(ci, size), 2))
        return (device, a)

    groups = [[xor(1, v) for v in (1, 2, 3)]]
    if nchain >= 64:
        groups.append([xor(4, v) for v in (1, 2, 3)])
    if nchain >= 16:
        groups.append([xor(3, 1)])
    groups += [[twin], [mate]]
    polar_peers = [device for group in groups for device in group]

    def remote(src, dst, number, device):
        return pltpu.make_async_remote_copy(
            src_ref=src,
            dst_ref=dst,
            send_sem=send_sem.at[number],
            recv_sem=recv_sem.at[number],
            device_id=device,
            device_id_type=MESH,
        )

    own_copies = [
        pltpu.make_async_copy(occ_hbm, halo.at[2, 0], local_sem.at[0]),
        pltpu.make_async_copy(vir_hbm, halo.at[2, 1], local_sem.at[1]),
    ]
    slab_copies = [
        pltpu.make_async_copy(
            tc_hbm.at[:, chunks * a + g], s_buf.at[g, pl.ds(half * a, half)], local_sem.at[2 + g]
        )
        for g in range(chunks)
    ]
    table_copies = [
        pltpu.make_async_copy(src, dst, local_sem.at[2 + chunks + n])
        for n, (src, dst) in enumerate(
            ((kern_hbm, kern_ref), (profile_hbm, profile_ref), (atom_hbm, atom_ref))
        )
    ]

    for slot, c0, n in ((0, 3, 6), (1, 1, 2), (2, 0, 1), (2, 8, 1), (3, 6, 2), (4, 0, 6)):
        pair_in[slot, :, pl.ds(c0 * B, n * B)] = jnp.zeros((B, n * B), BF16)

    barrier = pltpu.get_barrier_semaphore()
    greeted = [up, down] + polar_peers
    for device in greeted:
        pl.semaphore_signal(barrier, inc=1, device_id=device, device_id_type=MESH)
    for copy in own_copies + table_copies + slab_copies:
        copy.start()
    for copy in table_copies:
        copy.wait()
    row_id = lax.broadcasted_iota(jnp.int32, (half, B), 0)
    screen = jnp.zeros((half, B), F32)
    for p in range(half):
        near = jnp.abs(atom_ref[p] - ci) <= reach
        screen = jnp.where(row_id == p, jnp.where(near, 1.0, 0.0).astype(F32), screen)
    info[a, 0] = jnp.zeros((half, B), F32)
    info[a, 0, :, pl.ds(0, naux)] = kern_ref[...].astype(F32)
    info[a, 1] = screen
    pl.semaphore_wait(barrier, len(greeted))

    info_copy = remote(info.at[a], info.at[a], INFO, twin)
    for g in range(chunks):
        remote(
            tc_hbm.at[:, chunks * (1 - a) + g],
            s_buf.at[g, pl.ds(half * a, half)],
            S_IN + g,
            twin,
        ).start()
        if g == 0:
            info_copy.start()
    for copy in own_copies:
        copy.wait()
    up1 = remote(halo.at[2, :, :, pl.ds(B, 8 * B)], halo.at[1, :, :, pl.ds(B, 8 * B)], UP1, up)
    down1 = remote(halo.at[2, :, :, pl.ds(0, 8 * B)], halo.at[3, :, :, pl.ds(0, 8 * B)], DOWN1, down)
    up1.start()
    down1.start()
    up2 = remote(halo.at[1, :, :, pl.ds(3 * B, 6 * B)], halo.at[0, :, :, pl.ds(3 * B, 6 * B)], UP2, up)
    down2 = remote(halo.at[3, :, :, pl.ds(0, 6 * B)], halo.at[4, :, :, pl.ds(0, 6 * B)], DOWN2, down)
    pair_cols = ((3, 6), (1, 8), (0, 8), (0, 6))
    pair_copies = []
    for q in range(4):
        cols = pl.ds(pair_cols[q][0] * B, pair_cols[q][1] * B)
        pair_copies.append(
            remote(
                halo.at[q + 1 - core, :, :, cols], pair_halo.at[q, :, :, cols], PAIR + q, mate
            )
        )

    gram[...] = jnp.zeros_like(gram)
    coupled[...] = jnp.zeros_like(coupled)
    partner[...] = jnp.zeros_like(partner)
    terms[...] = jnp.zeros_like(terms)
    x_buf[...] = jnp.zeros_like(x_buf)
    v_buf[...] = jnp.zeros_like(v_buf)

    widths = []
    for t in range(SLOTS):
        block = ci + t - 4
        inside = (block >= 0) & (block < nchain)
        width = profile_ref[jnp.clip(block, 0, nchain - 1)]
        widths.append(jnp.where(inside, width, -1))
    row_ok = [jnp.abs(k - 4) <= jnp.minimum(widths[4], widths[k]) for k in range(SLOTS)]
    keep = [jnp.where(ok, 1.0, 0.0).astype(F32) for ok in row_ok]

    def assemble(d):
        k = d + 4
        for which, target in ((0, x_buf), (1, v_buf)):
            for c in range(max(0, d), min(8, 8 + d) + 1):
                ok = row_ok[k] & (abs(c - k) <= jnp.minimum(widths[k], widths[c]))
                factor = jnp.where(ok, 1.0, 0.0).astype(F32)
                cols = pl.ds((c - d) * B, B)
                if d % 2 == 0:
                    block = halo[2 + d // 2, which, :, cols]
                else:
                    block = pair_halo[(d + 3) // 2, which, :, cols]
                block = (block.astype(F32) * factor).astype(BF16)
                if c == 8:
                    xv_last[pl.ds((k - 4) * B, B), pl.ds(which * B, B)] = block
                else:
                    target[pl.ds(k * B, B), pl.ds(c * B, B)] = block

    assemble(0)
    up1.wait_recv()
    up2.start()
    down1.wait_recv()
    down2.start()
    pair_copies[1].start()
    pair_copies[2].start()

    @pl.when(core == 0)
    def _():
        pair_copies[0].start()

    @pl.when(core == 1)
    def _():
        pair_copies[3].start()

    assemble(-2)
    assemble(2)

    info_copy.wait_recv()
    tall = naux * ROWS
    lane = lax.broadcasted_iota(jnp.int32, (tall, B), 1)
    tall_row = lax.broadcasted_iota(jnp.int32, (tall, B), 0)
    pick = jnp.where(lax.div(tall_row, ROWS) == lane, 1.0, 0.0).astype(F32)
    kern_all = info[:, 0].reshape(naux, B)
    screen_all = info[:, 1].reshape(naux, B)
    screen_tall = jnp.broadcast_to(screen_all[:, None, :], (naux, ROWS, B)).reshape(tall, B)
    kern_tall = jnp.broadcast_to((kern_all * screen_all)[:, None, :], (naux, ROWS, B)).reshape(tall, B)
    spread = lax.dot_general(
        kern_tall.astype(BF16),
        (pick * screen_tall).astype(BF16),
        (((1,), (1,)), ((), ())),
        preferred_element_type=F32,
    )
    same_row = lax.rem(lax.broadcasted_iota(jnp.int32, (tall, tall), 0), ROWS) == lax.rem(
        lax.broadcasted_iota(jnp.int32, (tall, tall), 1), ROWS
    )
    kron[...] = jnp.where(same_row, spread, 0.0).astype(BF16)

    up2.wait_recv()
    down2.wait_recv()

    @pl.when(core == 1)
    def _():
        pair_copies[0].start()

    @pl.when(core == 0)
    def _():
        pair_copies[3].start()

    assemble(-4)
    assemble(4)
    for q, d in ((1, -1), (2, 1), (0, -3), (3, 3)):
        pair_copies[q].wait_recv()
        assemble(d)

    def add_gram():
        gram[...] += lax.dot_general(
            coupled[...], partner[...], (((1,), (1,)), ((), ())), preferred_element_type=F32
        )

    def products(g, slab):
        mine = pl.ds(half * slab, half)
        short = half * ROWS
        tall_rows = pl.ds(pl.multiple_of(short * slab, short), short)

        def cut(k0, k1):
            return s_buf[g, mine, :, pl.ds(k0 * B, (k1 - k0) * B)].reshape(short, (k1 - k0) * B)

        for c0, c1, k0, k1 in TILES:
            cols = pl.ds(c0 * B, (c1 - c0) * B)
            rows = pl.ds(k0 * B, (k1 - k0) * B)
            coupled[tall_rows, cols] = jnp.dot(cut(k0, k1), x_buf[rows, cols], preferred_element_type=F32).astype(BF16)
            partner[tall_rows, cols] = jnp.dot(cut(k0, k1), v_buf[rows, cols], preferred_element_type=F32).astype(BF16)
        last = jnp.dot(cut(4, 9), xv_last[...], preferred_element_type=F32).astype(BF16)
        coupled[tall_rows, pl.ds(8 * B, B)] = last[:, :B]
        partner[tall_rows, pl.ds(8 * B, B)] = last[:, B:]

    def step(g, carry):
        pltpu.make_async_copy(
            tc_hbm.at[:, chunks * a + g], s_buf.at[g, pl.ds(half * a, half)], local_sem.at[2 + g]
        ).wait()
        products(g, a)
        remote(
            tc_hbm.at[:, chunks * (1 - a) + g],
            s_buf.at[g, pl.ds(half * (1 - a), half)],
            S_IN + g,
            twin,
        ).wait_recv()
        products(g, 1 - a)
        add_gram()
        response[...] = jnp.dot(kron[...], partner[...], preferred_element_type=F32).astype(BF16)
        s_t[...] = s_buf[g].reshape(tall, W).T
        for c0, c1, k0, k1 in TILES + ((8, 9, 4, 9),):
            cols = pl.ds(c0 * B, (c1 - c0) * B)
            rows = pl.ds(k0 * B, (k1 - k0) * B)
            terms[rows, cols] += jnp.dot(s_t[rows, :], response[:, cols], preferred_element_type=F32)
        return carry

    lax.fori_loop(0, chunks, step, 0)

    def own_terms(p, run, d, cj, n=1):
        k = d + 4
        return terms[pl.ds(k * B + run * (B // 2) + p * RUN, RUN), pl.ds((cj + d) * B, n * B)] * keep[k]

    def mates(p, run, slot, cj):
        return pair_in[slot, pl.ds((2 * p + run) * RUN, RUN), pl.ds(cj * B, B)].astype(F32)

    def piece(p):
        return pl.ds(2 * p * RUN, 2 * RUN)

    gpair = [[None] * 4 for _ in range(PIECES)]
    for p in range(PIECES):
        for q in (0, 3, 1, 2):
            c0, n = pair_cols[q]
            cols = pl.ds(c0 * B, n * B)
            for run in (0, 1):
                pair_out[q, pl.ds((2 * p + run) * RUN, RUN), cols] = own_terms(p, run, 2 * q - 3, c0, n).astype(BF16)
            gpair[p][q] = remote(
                pair_out.at[q, piece(p), cols],
                pair_in.at[q + core, piece(p), cols],
                GPAIR + 4 * p + q,
                mate,
            )
            gpair[p][q].start()

    folded = jnp.where(same_row, gram[...], 0.0).reshape(naux, ROWS, tall).sum(1)
    polar = jnp.dot(folded, pick, preferred_element_type=F32, precision=lax.Precision.HIGHEST)
    square_row = lax.broadcasted_iota(jnp.int32, (naux, B), 0)
    square_lane = lax.broadcasted_iota(jnp.int32, (naux, B), 1)
    screen_lane = jnp.sum(jnp.where(square_row == square_lane, screen_all, 0.0), axis=0, keepdims=True)
    polar = polar * screen_all * screen_lane
    packed = polar[:8]
    for n in range(1, naux // 8):
        packed = packed + pltpu.roll(polar[8 * n : 8 * n + 8], n * naux, 1)
    pol_out[0] = packed
    pol_copies = []
    for r, group in enumerate(groups):
        first = sum(len(g) for g in groups[:r])
        pol_copies.append(
            [
                remote(pol_out.at[r], pol_in.at[first + n], POLAR + first + n, device)
                for n, device in enumerate(group)
            ]
        )

    def polar_start(r):
        for copy in pol_copies[r]:
            copy.start()

    def polar_round(r):
        for copy in pol_copies[r]:
            copy.wait_recv()
        first = sum(len(g) for g in groups[:r])
        value = pol_out[r] + pol_in[first]
        if len(groups[r]) == 3:
            value = value + (pol_in[first + 1] + pol_in[first + 2])
        pol_out[r + 1] = value
        if r + 1 < len(groups):
            polar_start(r + 1)

    ahead = list(range(len(groups) - 1))

    def advance():
        if ahead:
            polar_round(ahead.pop(0))

    polar_start(0)
    gup2, gdown2, gup1, gdown1, gaux = [], [], [], [], []
    for p in range(PIECES):
        for q in (0, 3, 1, 2):
            gpair[p][q].wait_recv()
        for run in (0, 1):
            at = pl.ds((2 * p + run) * RUN, RUN)
            for c in range(6):
                part = mates(p, run, 4, c)
                if c < 5:
                    part = part + own_terms(p, run, 4, c)
                out2[0, at, pl.ds(c * B, B)] = part.astype(BF16)
        gup2.append(remote(out2.at[0, piece(p)], in2.at[0, piece(p)], GUP2 + p, up))
        gup2[p].start()
        for run in (0, 1):
            at = pl.ds((2 * p + run) * RUN, RUN)
            for c in range(6):
                part = mates(p, run, 0, c + 3)
                if c >= 1:
                    part = part + own_terms(p, run, -4, c + 3)
                out2[1, at, pl.ds(c * B, B)] = part.astype(BF16)
        gdown2.append(remote(out2.at[1, piece(p)], in2.at[1, piece(p)], GDOWN2 + p, down))
        gdown2[p].start()

    advance()
    for p in range(PIECES):
        gup2[p].wait_recv()
        for run in (0, 1):
            at = pl.ds((2 * p + run) * RUN, RUN)
            for c in range(8):
                part = mates(p, run, 3, c)
                if c < 7:
                    part = part + own_terms(p, run, 2, c)
                if c < 6:
                    part = part + in2[0, at, pl.ds(c * B, B)].astype(F32)
                out1[0, at, pl.ds(c * B, B)] = part.astype(BF16)
        gup1.append(remote(out1.at[0, piece(p)], in1.at[0, piece(p)], GUP1 + p, up))
        gup1[p].start()
        gdown2[p].wait_recv()
        for run in (0, 1):
            at = pl.ds((2 * p + run) * RUN, RUN)
            for c in range(8):
                part = mates(p, run, 1, c + 1)
                if c >= 1:
                    part = part + own_terms(p, run, -2, c + 1)
                if c >= 2:
                    part = part + in2[1, at, pl.ds((c - 2) * B, B)].astype(F32)
                out1[1, at, pl.ds(c * B, B)] = part.astype(BF16)
        gdown1.append(remote(out1.at[1, piece(p)], in1.at[1, piece(p)], GDOWN1 + p, down))
        gdown1[p].start()
        advance()
    for p in range(PIECES):
        gup1[p].wait_recv()
        gdown1[p].wait_recv()
        for run in (0, 1):
            at = pl.ds((2 * p + run) * RUN, RUN)
            for c in range(SLOTS):
                part = mates(p, run, 2, c) + own_terms(p, run, 0, c)
                if c < 8:
                    part = part + in1[0, at, pl.ds(c * B, B)].astype(F32)
                if c >= 1:
                    part = part + in1[1, at, pl.ds((c - 1) * B, B)].astype(F32)
                total[run, pl.ds(p * RUN, RUN), pl.ds(c * B, B)] = part
        there = pl.ds(p * RUN, RUN)
        aux_out[there, :] = total[1 - a, there, :].astype(BF16)
        gaux.append(remote(aux_out.at[there], aux_in.at[there], GAUX + p, twin))
        gaux[p].start()
        advance()
    for p in range(PIECES):
        gaux[p].wait_recv()
        there = pl.ds(p * RUN, RUN)
        for c in range(SLOTS):
            cols = pl.ds(c * B, B)
            grad_ref[there, cols] = (
                total[a, there, cols] + aux_in[there, cols].astype(F32)
            ) * (keep[c] * scale_grad)
    polar_round(len(groups) - 1)
    packed = pol_out[len(groups)] * scale_pol
    for n in range(half // 8):
        here = [pltpu.roll(packed, (B - (n + slab * half // 8) * naux) % B, 1) for slab in (0, 1)]
        pol_ref[pl.ds(8 * n, 8), :] = jnp.where(a == 0, here[0], here[1])[:, :naux]

    info_copy.wait_send()
    for g in range(chunks):
        remote(
            tc_hbm.at[:, chunks * (1 - a) + g],
            s_buf.at[g, pl.ds(half * a, half)],
            S_IN + g,
            twin,
        ).wait_send()
    sent = [up1, down1, up2, down2] + pair_copies + gup2 + gdown2 + gup1 + gdown1 + gaux
    for copy in sent + [copy for group in gpair + pol_copies for copy in group]:
        copy.wait_send()


def body(occupied, virtual, three_centre, kern, profile, atom_map):
    nchain = lax.axis_size("chain")
    half = three_centre.shape[0]
    naux = kern.shape[1]
    chunks = (B // 2) // ROWS
    tall = naux * ROWS
    polars = 5 + 3 * (nchain >= 64) + (nchain >= 16)
    rounds = 3 + (nchain >= 64) + (nchain >= 16)
    slabs = three_centre.reshape(half, B // ROWS, ROWS, W)
    hbm = pl.BlockSpec(memory_space=pltpu.HBM)
    vmem = pl.BlockSpec(memory_space=pltpu.VMEM)
    grad, pol = pl.pallas_call(
        functools.partial(
            kernel,
            nchain,
            naux,
            nchain // 4,
            1.0 / math.sqrt(B * naux),
            1.0 / math.sqrt(B * nchain * W),
        ),
        out_shape=(
            jax.ShapeDtypeStruct((B // 2, W), F32),
            jax.ShapeDtypeStruct((half, naux), F32),
        ),
        in_specs=[hbm] * 6,
        out_specs=(vmem, vmem),
        scratch_shapes=[
            pltpu.VMEM((chunks, naux, ROWS, W), BF16),
            pltpu.VMEM((5, 2, B, W), BF16),
            pltpu.VMEM((4, 2, B, W), BF16),
            pltpu.VMEM((W, W), BF16),
            pltpu.VMEM((W, W), BF16),
            pltpu.VMEM((5 * B, 2 * B), BF16),
            pltpu.VMEM((W, tall), BF16),
            pltpu.VMEM((tall, W), BF16),
            pltpu.VMEM((tall, W), BF16),
            pltpu.VMEM((tall, W), BF16),
            pltpu.VMEM((tall, tall), F32),
            pltpu.VMEM((tall, tall), BF16),
            pltpu.VMEM((2, 2, half, B), F32),
            pltpu.VMEM((W, W), F32),
            pltpu.VMEM((4, B, W), BF16),
            pltpu.VMEM((5, B, W), BF16),
            pltpu.VMEM((2, B, 6 * B), BF16),
            pltpu.VMEM((2, B, 6 * B), BF16),
            pltpu.VMEM((2, B, 8 * B), BF16),
            pltpu.VMEM((2, B, 8 * B), BF16),
            pltpu.VMEM((2, B // 2, W), F32),
            pltpu.VMEM((B // 2, W), BF16),
            pltpu.VMEM((B // 2, W), BF16),
            pltpu.VMEM((rounds + 1, 8, B), F32),
            pltpu.VMEM((polars, 8, B), F32),
            pltpu.VMEM((half, naux), BF16),
            pltpu.SMEM((nchain,), jnp.int32),
            pltpu.SMEM((half,), jnp.int32),
            pltpu.SemaphoreType.DMA((POLAR + polars,)),
            pltpu.SemaphoreType.DMA((POLAR + polars,)),
            pltpu.SemaphoreType.DMA((5 + chunks,)),
        ],
        compiler_params=pltpu.CompilerParams(
            collective_id=0, has_side_effects=True, vmem_limit_bytes=VMEM_LIMIT
        ),
        name="rpa",
    )(*[pltpu.with_memory_space_constraint(x, pltpu.HBM) for x in (occupied, virtual, slabs, kern, profile, atom_map)])
    return grad, pol


def solution(mesh):
    placed = (
        P("chain", None),
        P("chain", None),
        P("aux", "chain", None),
        P("aux", None),
        P(),
        P("aux"),
    )
    return jax.shard_map(
        body,
        mesh=mesh,
        in_specs=placed,
        out_specs=(P(("chain", "aux"), None), P("aux", None)),
        check_vma=False,
    )
```

```python
import functools
import math

import jax
import jax.numpy as jnp
from jax import lax
from jax.experimental import pallas as pl
from jax.experimental.pallas import tpu as pltpu
from jax.sharding import PartitionSpec as P

MESH = pl.DeviceIdType.MESH
BF16 = jnp.bfloat16
F32 = jnp.float32
B = 128
SLOTS = 9
W = SLOTS * B
ROWS = 16
TILES = ((0, 2, 0, 6), (2, 4, 0, 8), (4, 6, 0, 9), (6, 8, 2, 9))

S_IN = 0
UP1, DOWN1, UP2, DOWN2 = 4, 5, 6, 7
PAIR = 8
INFO = 12
GPAIR = 13
PIECES = 2
RUN = B // (2 * PIECES)
GUP2, GDOWN2, GUP1, GDOWN1, GAUX, POLAR = [GPAIR + n * PIECES for n in (4, 5, 6, 8, 10, 11)]
VMEM_LIMIT = 44 * 2**20


def kernel(
    nchain,
    naux,
    reach,
    scale_grad,
    scale_pol,
    occ_hbm,
    vir_hbm,
    tc_hbm,
    kern_hbm,
    profile_hbm,
    atom_hbm,
    grad_ref,
    pol_ref,
    s_buf,
    halo,
    pair_halo,
    x_buf,
    v_buf,
    xv_last,
    s_t,
    coupled,
    partner,
    response,
    gram,
    kron,
    info,
    terms,
    pair_out,
    pair_in,
    out2,
    in2,
    out1,
    in1,
    total,
    aux_out,
    aux_in,
    pol_out,
    pol_in,
    kern_ref,
    profile_ref,
    atom_ref,
    send_sem,
    recv_sem,
    local_sem,
):
    half = naux // 2
    chunks = (B // 2) // ROWS
    chips = nchain // 2
    ci = lax.axis_index("chain")
    a = lax.axis_index("aux")
    chip = lax.div(ci, 2)
    core = lax.rem(ci, 2)
    inrow = lax.rem(chip, 4)
    flip_up = lax.div(inrow + 1, 4)
    flip_down = 1 - lax.div(inrow + 3, 4)
    up = (2 * lax.rem(chip + 1, chips) + core, lax.rem(a + flip_up, 2))
    down = (2 * lax.rem(chip + chips - 1, chips) + core, lax.rem(a + flip_down, 2))
    up_twin = (up[0], 1 - up[1])
    down_twin = (down[0], 1 - down[1])
    mate = (2 * chip + 1 - core, a)
    twin = (ci, 1 - a)

    def across(bit):
        size = 1 << bit
        return (ci + size * (1 - 2 * lax.rem(lax.div(ci, size), 2)), a)

    def xor(low, value):
        device = ci
        for bit in (0, 1):
            if value >> bit & 1:
                size = 1 << (low + bit)
                device = device + size * (1 - 2 * lax.rem(lax.div(ci, size), 2))
        return (device, a)

    groups = [[xor(1, v) for v in (1, 2, 3)], [twin]]
    if nchain >= 64:
        groups.append([xor(4, v) for v in (1, 2, 3)])
    if nchain >= 16:
        groups.append([xor(3, 1)])
    groups += [[mate]]
    polar_peers = [device for group in groups for device in group]

    def remote(src, dst, number, device):
        return pltpu.make_async_remote_copy(
            src_ref=src,
            dst_ref=dst,
            send_sem=send_sem.at[number],
            recv_sem=recv_sem.at[number],
            device_id=device,
            device_id_type=MESH,
        )

    own_copies = [
        pltpu.make_async_copy(occ_hbm, halo.at[2, 0], local_sem.at[0]),
        pltpu.make_async_copy(vir_hbm, halo.at[2, 1], local_sem.at[1]),
    ]
    slab_copies = [
        pltpu.make_async_copy(
            tc_hbm.at[:, chunks * a + g], s_buf.at[g, pl.ds(half * a, half)], local_sem.at[2 + g]
        )
        for g in range(chunks)
    ]
    table_copies = [
        pltpu.make_async_copy(src, dst, local_sem.at[2 + chunks + n])
        for n, (src, dst) in enumerate(
            ((kern_hbm, kern_ref), (profile_hbm, profile_ref), (atom_hbm, atom_ref))
        )
    ]

    for slot, c0, n in ((0, 3, 6), (1, 1, 2), (2, 0, 1), (2, 8, 1), (3, 6, 2), (4, 0, 6)):
        pair_in[slot, :, pl.ds(c0 * B, n * B)] = jnp.zeros((B, n * B), BF16)

    barrier = pltpu.get_barrier_semaphore()
    greeted = [up, down, up_twin, down_twin] + polar_peers
    for device in greeted:
        pl.semaphore_signal(barrier, inc=1, device_id=device, device_id_type=MESH)
    for copy in own_copies + table_copies + slab_copies:
        copy.start()
    for copy in table_copies:
        copy.wait()
    row_id = lax.broadcasted_iota(jnp.int32, (half, B), 0)
    screen = jnp.zeros((half, B), F32)
    for p in range(half):
        near = jnp.abs(atom_ref[p] - ci) <= reach
        screen = jnp.where(row_id == p, jnp.where(near, 1.0, 0.0).astype(F32), screen)
    info[a, 0] = jnp.zeros((half, B), F32)
    info[a, 0, :, pl.ds(0, naux)] = kern_ref[...].astype(F32)
    info[a, 1] = screen
    pl.semaphore_wait(barrier, len(greeted))

    info_copy = remote(info.at[a], info.at[a], INFO, twin)
    for g in range(chunks):
        remote(
            tc_hbm.at[:, chunks * (1 - a) + g],
            s_buf.at[g, pl.ds(half * a, half)],
            S_IN + g,
            twin,
        ).start()
        if g == 0:
            info_copy.start()
    for copy in own_copies:
        copy.wait()
    up1 = remote(halo.at[2, :, :, pl.ds(B, 8 * B)], halo.at[1, :, :, pl.ds(B, 8 * B)], UP1, up)
    down1 = remote(halo.at[2, :, :, pl.ds(0, 8 * B)], halo.at[3, :, :, pl.ds(0, 8 * B)], DOWN1, down)
    up1.start()
    down1.start()
    up2 = remote(halo.at[1, :, :, pl.ds(3 * B, 6 * B)], halo.at[0, :, :, pl.ds(3 * B, 6 * B)], UP2, up)
    down2 = remote(halo.at[3, :, :, pl.ds(0, 6 * B)], halo.at[4, :, :, pl.ds(0, 6 * B)], DOWN2, down)
    pair_cols = ((3, 6), (1, 8), (0, 8), (0, 6))
    pair_copies = []
    for q in range(4):
        cols = pl.ds(pair_cols[q][0] * B, pair_cols[q][1] * B)
        pair_copies.append(
            remote(
                halo.at[q + 1 - core, :, :, cols], pair_halo.at[q, :, :, cols], PAIR + q, mate
            )
        )

    gram[...] = jnp.zeros_like(gram)
    coupled[...] = jnp.zeros_like(coupled)
    partner[...] = jnp.zeros_like(partner)
    terms[...] = jnp.zeros_like(terms)
    x_buf[...] = jnp.zeros_like(x_buf)
    v_buf[...] = jnp.zeros_like(v_buf)

    widths = []
    for t in range(SLOTS):
        block = ci + t - 4
        inside = (block >= 0) & (block < nchain)
        width = profile_ref[jnp.clip(block, 0, nchain - 1)]
        widths.append(jnp.where(inside, width, -1))
    row_ok = [jnp.abs(k - 4) <= jnp.minimum(widths[4], widths[k]) for k in range(SLOTS)]
    keep = [jnp.where(ok, 1.0, 0.0).astype(F32) for ok in row_ok]

    def assemble(d):
        k = d + 4
        for which, target in ((0, x_buf), (1, v_buf)):
            for c in range(max(0, d), min(8, 8 + d) + 1):
                ok = row_ok[k] & (abs(c - k) <= jnp.minimum(widths[k], widths[c]))
                factor = jnp.where(ok, 1.0, 0.0).astype(F32)
                cols = pl.ds((c - d) * B, B)
                if d % 2 == 0:
                    block = halo[2 + d // 2, which, :, cols]
                else:
                    block = pair_halo[(d + 3) // 2, which, :, cols]
                block = (block.astype(F32) * factor).astype(BF16)
                if c == 8:
                    xv_last[pl.ds((k - 4) * B, B), pl.ds(which * B, B)] = block
                else:
                    target[pl.ds(k * B, B), pl.ds(c * B, B)] = block

    assemble(0)
    up1.wait_recv()
    up2.start()
    down1.wait_recv()
    down2.start()
    pair_copies[1].start()
    pair_copies[2].start()

    @pl.when(core == 0)
    def _():
        pair_copies[0].start()

    @pl.when(core == 1)
    def _():
        pair_copies[3].start()

    assemble(-2)
    assemble(2)

    info_copy.wait_recv()
    tall = naux * ROWS
    lane = lax.broadcasted_iota(jnp.int32, (tall, B), 1)
    tall_row = lax.broadcasted_iota(jnp.int32, (tall, B), 0)
    pick = jnp.where(lax.div(tall_row, ROWS) == lane, 1.0, 0.0).astype(F32)
    kern_all = info[:, 0].reshape(naux, B)
    screen_all = info[:, 1].reshape(naux, B)
    screen_tall = jnp.broadcast_to(screen_all[:, None, :], (naux, ROWS, B)).reshape(tall, B)
    kern_tall = jnp.broadcast_to((kern_all * screen_all)[:, None, :], (naux, ROWS, B)).reshape(tall, B)
    spread = lax.dot_general(
        kern_tall.astype(BF16),
        (pick * screen_tall).astype(BF16),
        (((1,), (1,)), ((), ())),
        preferred_element_type=F32,
    )
    same_row = lax.rem(lax.broadcasted_iota(jnp.int32, (tall, tall), 0), ROWS) == lax.rem(
        lax.broadcasted_iota(jnp.int32, (tall, tall), 1), ROWS
    )
    kron[...] = jnp.where(same_row, spread, 0.0).astype(BF16)

    up2.wait_recv()
    down2.wait_recv()

    @pl.when(core == 1)
    def _():
        pair_copies[0].start()

    @pl.when(core == 0)
    def _():
        pair_copies[3].start()

    assemble(-4)
    assemble(4)
    for q, d in ((1, -1), (2, 1), (0, -3), (3, 3)):
        pair_copies[q].wait_recv()
        assemble(d)

    def add_gram():
        gram[...] += lax.dot_general(
            coupled[...], partner[...], (((1,), (1,)), ((), ())), preferred_element_type=F32
        )

    def products(g, slab):
        mine = pl.ds(half * slab, half)
        short = half * ROWS
        tall_rows = pl.ds(pl.multiple_of(short * slab, short), short)

        def cut(k0, k1):
            return s_buf[g, mine, :, pl.ds(k0 * B, (k1 - k0) * B)].reshape(short, (k1 - k0) * B)

        for c0, c1, k0, k1 in TILES:
            cols = pl.ds(c0 * B, (c1 - c0) * B)
            rows = pl.ds(k0 * B, (k1 - k0) * B)
            coupled[tall_rows, cols] = jnp.dot(cut(k0, k1), x_buf[rows, cols], preferred_element_type=F32).astype(BF16)
            partner[tall_rows, cols] = jnp.dot(cut(k0, k1), v_buf[rows, cols], preferred_element_type=F32).astype(BF16)
        last = jnp.dot(cut(4, 9), xv_last[...], preferred_element_type=F32).astype(BF16)
        coupled[tall_rows, pl.ds(8 * B, B)] = last[:, :B]
        partner[tall_rows, pl.ds(8 * B, B)] = last[:, B:]

    def step(g, carry):
        pltpu.make_async_copy(
            tc_hbm.at[:, chunks * a + g], s_buf.at[g, pl.ds(half * a, half)], local_sem.at[2 + g]
        ).wait()
        products(g, a)
        remote(
            tc_hbm.at[:, chunks * (1 - a) + g],
            s_buf.at[g, pl.ds(half * (1 - a), half)],
            S_IN + g,
            twin,
        ).wait_recv()
        products(g, 1 - a)
        add_gram()
        response[...] = jnp.dot(kron[...], partner[...], preferred_element_type=F32).astype(BF16)
        s_t[...] = s_buf[g].reshape(tall, W).T
        for c0, c1, k0, k1 in TILES + ((8, 9, 4, 9),):
            cols = pl.ds(c0 * B, (c1 - c0) * B)
            rows = pl.ds(k0 * B, (k1 - k0) * B)
            terms[rows, cols] += jnp.dot(s_t[rows, :], response[:, cols], preferred_element_type=F32)
        return carry

    lax.fori_loop(0, chunks, step, 0)

    def own_terms(p, run, d, cj, n=1):
        k = d + 4
        return terms[pl.ds(k * B + run * (B // 2) + p * RUN, RUN), pl.ds((cj + d) * B, n * B)] * keep[k]

    def mates(p, run, slot, cj):
        return pair_in[slot, pl.ds((2 * p + run) * RUN, RUN), pl.ds(cj * B, B)].astype(F32)

    def piece(p):
        return pl.ds(2 * p * RUN, 2 * RUN)

    gpair = [[None] * 4 for _ in range(PIECES)]
    for p in range(PIECES):
        for q in (0, 3, 1, 2):
            c0, n = pair_cols[q]
            cols = pl.ds(c0 * B, n * B)
            for run in (0, 1):
                pair_out[q, pl.ds((2 * p + run) * RUN, RUN), cols] = own_terms(p, run, 2 * q - 3, c0, n).astype(BF16)
            gpair[p][q] = remote(
                pair_out.at[q, piece(p), cols],
                pair_in.at[q + core, piece(p), cols],
                GPAIR + 4 * p + q,
                mate,
            )
            gpair[p][q].start()

    folded = jnp.where(same_row, gram[...], 0.0).reshape(naux, ROWS, tall).sum(1)
    polar = jnp.dot(folded, pick, preferred_element_type=F32, precision=lax.Precision.HIGHEST)
    square_row = lax.broadcasted_iota(jnp.int32, (naux, B), 0)
    square_lane = lax.broadcasted_iota(jnp.int32, (naux, B), 1)
    screen_lane = jnp.sum(jnp.where(square_row == square_lane, screen_all, 0.0), axis=0, keepdims=True)
    polar = polar * screen_all * screen_lane
    packed = polar[:8]
    for n in range(1, naux // 8):
        packed = packed + pltpu.roll(polar[8 * n : 8 * n + 8], n * naux, 1)
    pol_out[0] = packed
    pol_copies = []
    for r, group in enumerate(groups):
        first = sum(len(g) for g in groups[:r])
        pol_copies.append(
            [
                remote(pol_out.at[r], pol_in.at[first + n], POLAR + first + n, device)
                for n, device in enumerate(group)
            ]
        )

    def polar_start(r):
        for copy in pol_copies[r]:
            copy.start()

    def polar_round(r):
        for copy in pol_copies[r]:
            copy.wait_recv()
        first = sum(len(g) for g in groups[:r])
        value = pol_out[r] + pol_in[first]
        if len(groups[r]) == 3:
            value = value + (pol_in[first + 1] + pol_in[first + 2])
        pol_out[r + 1] = value
        if r + 1 < len(groups):
            polar_start(r + 1)

    ahead = list(range(len(groups) - 1))

    def advance():
        if ahead:
            polar_round(ahead.pop(0))

    polar_start(0)
    gup2, gdown2, gup1, gdown1, gaux = [], [], [], [], []
    for p in range(PIECES):
        for q in (0, 3, 1, 2):
            gpair[p][q].wait_recv()
        for run in (0, 1):
            at = pl.ds((2 * p + run) * RUN, RUN)
            for c in range(6):
                part = mates(p, run, 4, c)
                if c < 5:
                    part = part + own_terms(p, run, 4, c)
                out2[0, at, pl.ds(c * B, B)] = part.astype(BF16)
        gup2.append(remote(out2.at[0, piece(p)], in2.at[0, piece(p)], GUP2 + p, up))
        gup2[p].start()
        for run in (0, 1):
            at = pl.ds((2 * p + run) * RUN, RUN)
            for c in range(6):
                part = mates(p, run, 0, c + 3)
                if c >= 1:
                    part = part + own_terms(p, run, -4, c + 3)
                out2[1, at, pl.ds(c * B, B)] = part.astype(BF16)
        gdown2.append(remote(out2.at[1, piece(p)], in2.at[1, piece(p)], GDOWN2 + p, down))
        gdown2[p].start()

    advance()

    for p in range(PIECES):
        for run in (0, 1):
            for c in range(SLOTS):
                total[run, pl.ds(p * RUN, RUN), pl.ds(c * B, B)] = mates(p, run, 2, c) + own_terms(p, run, 0, c)
    aux_out[...] = total[1 - a].astype(BF16)
    gaux.append(remote(aux_out, aux_in, GAUX, twin))
    gaux[0].start()

    def last_hop(way, number, p, near, far):
        copies = []
        for kind, device in enumerate((near, far)):
            copies.append(
                remote(out1.at[way, p, device[1]], in1.at[way, kind, p], number + 2 * p + kind, device)
            )
            copies[kind].start()
        return copies

    for p in range(PIECES):
        gup2[p].wait_recv()
        for run in (0, 1):
            at = pl.ds((2 * p + run) * RUN, RUN)
            for c in range(8):
                part = mates(p, run, 3, c)
                if c < 7:
                    part = part + own_terms(p, run, 2, c)
                if c < 6:
                    part = part + in2[0, at, pl.ds(c * B, B)].astype(F32)
                out1[0, p, run, :, pl.ds(c * B, B)] = part.astype(BF16)
        gup1.append(last_hop(0, GUP1, p, up, up_twin))
        gdown2[p].wait_recv()
        for run in (0, 1):
            at = pl.ds((2 * p + run) * RUN, RUN)
            for c in range(8):
                part = mates(p, run, 1, c + 1)
                if c >= 1:
                    part = part + own_terms(p, run, -2, c + 1)
                if c >= 2:
                    part = part + in2[1, at, pl.ds((c - 2) * B, B)].astype(F32)
                out1[1, p, run, :, pl.ds(c * B, B)] = part.astype(BF16)
        gdown1.append(last_hop(1, GDOWN1, p, down, down_twin))
        advance()
    while ahead:
        advance()
    gaux[0].wait_recv()
    for p in range(PIECES):
        for copy in gup1[p] + gdown1[p]:
            copy.wait_recv()
        there = pl.ds(p * RUN, RUN)
        for c in range(SLOTS):
            cols = pl.ds(c * B, B)
            part = total[a, there, cols] + aux_in[there, cols].astype(F32)
            for kind in (0, 1):
                if c < 8:
                    part = part + in1[0, kind, p, :, cols].astype(F32)
                if c >= 1:
                    part = part + in1[1, kind, p, :, pl.ds((c - 1) * B, B)].astype(F32)
            grad_ref[there, cols] = part * (keep[c] * scale_grad)
    polar_round(len(groups) - 1)
    packed = pol_out[len(groups)] * scale_pol
    for n in range(half // 8):
        here = [pltpu.roll(packed, (B - (n + slab * half // 8) * naux) % B, 1) for slab in (0, 1)]
        pol_ref[pl.ds(8 * n, 8), :] = jnp.where(a == 0, here[0], here[1])[:, :naux]

    info_copy.wait_send()
    for g in range(chunks):
        remote(
            tc_hbm.at[:, chunks * (1 - a) + g],
            s_buf.at[g, pl.ds(half * a, half)],
            S_IN + g,
            twin,
        ).wait_send()
    sent = [up1, down1, up2, down2] + pair_copies + gup2 + gdown2 + gaux
    for copy in sent + [copy for group in gpair + gup1 + gdown1 + pol_copies for copy in group]:
        copy.wait_send()


def body(occupied, virtual, three_centre, kern, profile, atom_map):
    nchain = lax.axis_size("chain")
    half = three_centre.shape[0]
    naux = kern.shape[1]
    chunks = (B // 2) // ROWS
    tall = naux * ROWS
    polars = 5 + 3 * (nchain >= 64) + (nchain >= 16)
    rounds = 3 + (nchain >= 64) + (nchain >= 16)
    slabs = three_centre.reshape(half, B // ROWS, ROWS, W)
    hbm = pl.BlockSpec(memory_space=pltpu.HBM)
    vmem = pl.BlockSpec(memory_space=pltpu.VMEM)
    grad, pol = pl.pallas_call(
        functools.partial(
            kernel,
            nchain,
            naux,
            nchain // 4,
            1.0 / math.sqrt(B * naux),
            1.0 / math.sqrt(B * nchain * W),
        ),
        out_shape=(
            jax.ShapeDtypeStruct((B // 2, W), F32),
            jax.ShapeDtypeStruct((half, naux), F32),
        ),
        in_specs=[hbm] * 6,
        out_specs=(vmem, vmem),
        scratch_shapes=[
            pltpu.VMEM((chunks, naux, ROWS, W), BF16),
            pltpu.VMEM((5, 2, B, W), BF16),
            pltpu.VMEM((4, 2, B, W), BF16),
            pltpu.VMEM((W, W), BF16),
            pltpu.VMEM((W, W), BF16),
            pltpu.VMEM((5 * B, 2 * B), BF16),
            pltpu.VMEM((W, tall), BF16),
            pltpu.VMEM((tall, W), BF16),
            pltpu.VMEM((tall, W), BF16),
            pltpu.VMEM((tall, W), BF16),
            pltpu.VMEM((tall, tall), F32),
            pltpu.VMEM((tall, tall), BF16),
            pltpu.VMEM((2, 2, half, B), F32),
            pltpu.VMEM((W, W), F32),
            pltpu.VMEM((4, B, W), BF16),
            pltpu.VMEM((5, B, W), BF16),
            pltpu.VMEM((2, B, 6 * B), BF16),
            pltpu.VMEM((2, B, 6 * B), BF16),
            pltpu.VMEM((2, PIECES, 2, RUN, 8 * B), BF16),
            pltpu.VMEM((2, 2, PIECES, RUN, 8 * B), BF16),
            pltpu.VMEM((2, B // 2, W), F32),
            pltpu.VMEM((B // 2, W), BF16),
            pltpu.VMEM((B // 2, W), BF16),
            pltpu.VMEM((rounds + 1, 8, B), F32),
            pltpu.VMEM((polars, 8, B), F32),
            pltpu.VMEM((half, naux), BF16),
            pltpu.SMEM((nchain,), jnp.int32),
            pltpu.SMEM((half,), jnp.int32),
            pltpu.SemaphoreType.DMA((POLAR + polars,)),
            pltpu.SemaphoreType.DMA((POLAR + polars,)),
            pltpu.SemaphoreType.DMA((5 + chunks,)),
        ],
        compiler_params=pltpu.CompilerParams(
            collective_id=0, has_side_effects=True, vmem_limit_bytes=VMEM_LIMIT
        ),
        name="rpa",
    )(*[pltpu.with_memory_space_constraint(x, pltpu.HBM) for x in (occupied, virtual, slabs, kern, profile, atom_map)])
    return grad, pol


def solution(mesh):
    placed = (
        P("chain", None),
        P("chain", None),
        P("aux", "chain", None),
        P("aux", None),
        P(),
        P("aux"),
    )
    return jax.shard_map(
        body,
        mesh=mesh,
        in_specs=placed,
        out_specs=(P(("chain", "aux"), None), P("aux", None)),
        check_vma=False,
    )
```

```python
import functools
import math

import jax
import jax.numpy as jnp
from jax import lax
from jax.experimental import pallas as pl
from jax.experimental.pallas import tpu as pltpu
from jax.sharding import PartitionSpec as P

MESH = pl.DeviceIdType.MESH
BF16 = jnp.bfloat16
F32 = jnp.float32
B = 128
SLOTS = 9
W = SLOTS * B
ROWS = 16
TILES = ((0, 2, 0, 6), (2, 4, 0, 8), (4, 6, 0, 9), (6, 8, 2, 9))

S_IN = 0
UP1, DOWN1, UP2, DOWN2 = 4, 5, 6, 7
PAIR = 8
INFO = 12
GPAIR = 13
PIECES = 2
RUN = B // (2 * PIECES)
GUP2, GDOWN2, GUP1, GDOWN1, GAUX, POLAR = [GPAIR + n * PIECES for n in (4, 5, 6, 8, 10, 11)]
VMEM_LIMIT = 44 * 2**20


def kernel(
    nchain,
    naux,
    reach,
    scale_grad,
    scale_pol,
    occ_hbm,
    vir_hbm,
    tc_hbm,
    kern_hbm,
    profile_hbm,
    atom_hbm,
    grad_ref,
    pol_ref,
    s_buf,
    halo,
    pair_halo,
    x_buf,
    v_buf,
    xv_last,
    s_t,
    coupled,
    partner,
    response,
    gram,
    kron,
    info,
    terms,
    pair_out,
    pair_in,
    out2,
    in2,
    out1,
    in1,
    total,
    aux_out,
    aux_in,
    pol_out,
    pol_in,
    kern_ref,
    profile_ref,
    atom_ref,
    send_sem,
    recv_sem,
    local_sem,
):
    half = naux // 2
    chunks = (B // 2) // ROWS
    chips = nchain // 2
    ci = lax.axis_index("chain")
    a = lax.axis_index("aux")
    chip = lax.div(ci, 2)
    core = lax.rem(ci, 2)
    inrow = lax.rem(chip, 4)
    flip_up = lax.div(inrow + 1, 4)
    flip_down = 1 - lax.div(inrow + 3, 4)
    up = (2 * lax.rem(chip + 1, chips) + core, lax.rem(a + flip_up, 2))
    down = (2 * lax.rem(chip + chips - 1, chips) + core, lax.rem(a + flip_down, 2))
    up_twin = (up[0], 1 - up[1])
    down_twin = (down[0], 1 - down[1])
    mate = (2 * chip + 1 - core, a)
    twin = (ci, 1 - a)

    def across(bit):
        size = 1 << bit
        return (ci + size * (1 - 2 * lax.rem(lax.div(ci, size), 2)), a)

    def xor(low, value):
        device = ci
        for bit in (0, 1):
            if value >> bit & 1:
                size = 1 << (low + bit)
                device = device + size * (1 - 2 * lax.rem(lax.div(ci, size), 2))
        return (device, a)

    groups = [[xor(1, v) for v in (1, 2, 3)], [twin]]
    if nchain >= 64:
        groups.append([xor(4, v) for v in (1, 2, 3)])
    if nchain >= 16:
        groups.append([xor(3, 1)])
    groups += [[mate]]
    polar_peers = [device for group in groups for device in group]

    def remote(src, dst, number, device):
        return pltpu.make_async_remote_copy(
            src_ref=src,
            dst_ref=dst,
            send_sem=send_sem.at[number],
            recv_sem=recv_sem.at[number],
            device_id=device,
            device_id_type=MESH,
        )

    class PerCore:
        def __init__(self, src, dst, number, device, spans):
            self.copies = [
                remote(src.at[:, pl.ds(c0 * B, n * B)], dst.at[:, pl.ds(c0 * B, n * B)], number, device)
                for c0, n in spans
            ]

        def each(self, act):
            for which, copy in enumerate(self.copies):
                pl.when(core == which)(functools.partial(act, copy))

        def start(self):
            self.each(lambda copy: copy.start())

        def wait_recv(self):
            self.each(lambda copy: copy.wait_recv())

        def wait_send(self):
            self.each(lambda copy: copy.wait_send())

    own_copies = [
        pltpu.make_async_copy(occ_hbm, halo.at[2, 0], local_sem.at[0]),
        pltpu.make_async_copy(vir_hbm, halo.at[2, 1], local_sem.at[1]),
    ]
    slab_copies = [
        pltpu.make_async_copy(
            tc_hbm.at[:, chunks * a + g], s_buf.at[g, pl.ds(half * a, half)], local_sem.at[2 + g]
        )
        for g in range(chunks)
    ]
    table_copies = [
        pltpu.make_async_copy(src, dst, local_sem.at[2 + chunks + n])
        for n, (src, dst) in enumerate(
            ((kern_hbm, kern_ref), (profile_hbm, profile_ref), (atom_hbm, atom_ref))
        )
    ]

    for slot, c0, n in ((0, 3, 6), (1, 1, 2), (2, 0, 1), (2, 8, 1), (3, 6, 2), (4, 0, 6)):
        pair_in[slot, :, pl.ds(c0 * B, n * B)] = jnp.zeros((B, n * B), BF16)

    in2[0, :, pl.ds(5 * B, B)] = jnp.zeros((B, B), BF16)
    in2[1, :, pl.ds(0, B)] = jnp.zeros((B, B), BF16)
    in1[0, :, :, :, pl.ds(7 * B, B)] = jnp.zeros((2, PIECES, RUN, B), BF16)
    in1[1, :, :, :, pl.ds(0, B)] = jnp.zeros((2, PIECES, RUN, B), BF16)

    barrier = pltpu.get_barrier_semaphore()
    greeted = [up, down, up_twin, down_twin] + polar_peers
    for device in greeted:
        pl.semaphore_signal(barrier, inc=1, device_id=device, device_id_type=MESH)
    for copy in own_copies + table_copies + slab_copies:
        copy.start()
    pl.semaphore_wait(barrier, len(greeted))

    def slab_out(g):
        return remote(
            tc_hbm.at[:, chunks * (1 - a) + g],
            s_buf.at[g, pl.ds(half * a, half)],
            S_IN + g,
            twin,
        )

    slab_out(0).start()
    for copy in table_copies:
        copy.wait()
    row_id = lax.broadcasted_iota(jnp.int32, (half, B), 0)
    screen = jnp.zeros((half, B), F32)
    for p in range(half):
        near = jnp.abs(atom_ref[p] - ci) <= reach
        screen = jnp.where(row_id == p, jnp.where(near, 1.0, 0.0).astype(F32), screen)
    info[a, 0] = jnp.zeros((half, B), F32)
    info[a, 0, :, pl.ds(0, naux)] = kern_ref[...].astype(F32)
    info[a, 1] = screen
    info_copy = remote(info.at[a], info.at[a], INFO, twin)
    info_copy.start()
    for g in range(1, chunks):
        slab_out(g).start()
    for copy in own_copies:
        copy.wait()
    up1 = remote(halo.at[2, :, :, pl.ds(B, 8 * B)], halo.at[1, :, :, pl.ds(B, 8 * B)], UP1, up)
    down1 = remote(halo.at[2, :, :, pl.ds(0, 8 * B)], halo.at[3, :, :, pl.ds(0, 8 * B)], DOWN1, down)
    up1.start()
    down1.start()
    up2 = remote(halo.at[1, :, :, pl.ds(3 * B, 6 * B)], halo.at[0, :, :, pl.ds(3 * B, 6 * B)], UP2, up)
    down2 = remote(halo.at[3, :, :, pl.ds(0, 6 * B)], halo.at[4, :, :, pl.ds(0, 6 * B)], DOWN2, down)
    pair_cols = ((3, 6), (1, 8), (0, 8), (0, 6))
    pair_copies = []
    for q in range(4):
        cols = pl.ds(pair_cols[q][0] * B, pair_cols[q][1] * B)
        pair_copies.append(
            remote(
                halo.at[q + 1 - core, :, :, cols], pair_halo.at[q, :, :, cols], PAIR + q, mate
            )
        )

    gram[...] = jnp.zeros_like(gram)
    coupled[...] = jnp.zeros_like(coupled)
    partner[...] = jnp.zeros_like(partner)
    terms[...] = jnp.zeros_like(terms)
    x_buf[...] = jnp.zeros_like(x_buf)
    v_buf[...] = jnp.zeros_like(v_buf)

    widths = []
    for t in range(SLOTS):
        block = ci + t - 4
        inside = (block >= 0) & (block < nchain)
        width = profile_ref[jnp.clip(block, 0, nchain - 1)]
        widths.append(jnp.where(inside, width, -1))
    row_ok = [jnp.abs(k - 4) <= jnp.minimum(widths[4], widths[k]) for k in range(SLOTS)]
    keep = [jnp.where(ok, 1.0, 0.0).astype(F32) for ok in row_ok]

    def assemble(d):
        k = d + 4
        for which, target in ((0, x_buf), (1, v_buf)):
            for c in range(max(0, d), min(8, 8 + d) + 1):
                ok = row_ok[k] & (abs(c - k) <= jnp.minimum(widths[k], widths[c]))
                factor = jnp.where(ok, 1.0, 0.0).astype(F32)
                cols = pl.ds((c - d) * B, B)
                if d % 2 == 0:
                    block = halo[2 + d // 2, which, :, cols]
                else:
                    block = pair_halo[(d + 3) // 2, which, :, cols]
                block = (block.astype(F32) * factor).astype(BF16)
                if c == 8:
                    xv_last[pl.ds((k - 4) * B, B), pl.ds(which * B, B)] = block
                else:
                    target[pl.ds(k * B, B), pl.ds(c * B, B)] = block

    assemble(0)
    up1.wait_recv()
    up2.start()
    down1.wait_recv()
    down2.start()
    pair_copies[1].start()
    pair_copies[2].start()

    @pl.when(core == 0)
    def _():
        pair_copies[0].start()

    @pl.when(core == 1)
    def _():
        pair_copies[3].start()

    assemble(-2)
    assemble(2)

    info_copy.wait_recv()
    tall = naux * ROWS
    lane = lax.broadcasted_iota(jnp.int32, (tall, B), 1)
    tall_row = lax.broadcasted_iota(jnp.int32, (tall, B), 0)
    pick = jnp.where(lax.div(tall_row, ROWS) == lane, 1.0, 0.0).astype(F32)
    kern_all = info[:, 0].reshape(naux, B)
    screen_all = info[:, 1].reshape(naux, B)
    screen_tall = jnp.broadcast_to(screen_all[:, None, :], (naux, ROWS, B)).reshape(tall, B)
    kern_tall = jnp.broadcast_to((kern_all * screen_all)[:, None, :], (naux, ROWS, B)).reshape(tall, B)
    spread = lax.dot_general(
        kern_tall.astype(BF16),
        (pick * screen_tall).astype(BF16),
        (((1,), (1,)), ((), ())),
        preferred_element_type=F32,
    )
    same_row = lax.rem(lax.broadcasted_iota(jnp.int32, (tall, tall), 0), ROWS) == lax.rem(
        lax.broadcasted_iota(jnp.int32, (tall, tall), 1), ROWS
    )
    kron[...] = jnp.where(same_row, spread, 0.0).astype(BF16)

    up2.wait_recv()
    down2.wait_recv()

    @pl.when(core == 1)
    def _():
        pair_copies[0].start()

    @pl.when(core == 0)
    def _():
        pair_copies[3].start()

    assemble(-4)
    assemble(4)
    for q, d in ((1, -1), (2, 1), (0, -3), (3, 3)):
        pair_copies[q].wait_recv()
        assemble(d)

    def add_gram():
        gram[...] += lax.dot_general(
            coupled[...], partner[...], (((1,), (1,)), ((), ())), preferred_element_type=F32
        )

    def products(g, slab):
        mine = pl.ds(half * slab, half)
        short = half * ROWS
        tall_rows = pl.ds(pl.multiple_of(short * slab, short), short)

        def cut(k0, k1):
            return s_buf[g, mine, :, pl.ds(k0 * B, (k1 - k0) * B)].reshape(short, (k1 - k0) * B)

        for c0, c1, k0, k1 in TILES:
            cols = pl.ds(c0 * B, (c1 - c0) * B)
            rows = pl.ds(k0 * B, (k1 - k0) * B)
            coupled[tall_rows, cols] = jnp.dot(cut(k0, k1), x_buf[rows, cols], preferred_element_type=F32).astype(BF16)
            partner[tall_rows, cols] = jnp.dot(cut(k0, k1), v_buf[rows, cols], preferred_element_type=F32).astype(BF16)
        last = jnp.dot(cut(4, 9), xv_last[...], preferred_element_type=F32).astype(BF16)
        coupled[tall_rows, pl.ds(8 * B, B)] = last[:, :B]
        partner[tall_rows, pl.ds(8 * B, B)] = last[:, B:]

    def step(g, carry):
        pltpu.make_async_copy(
            tc_hbm.at[:, chunks * a + g], s_buf.at[g, pl.ds(half * a, half)], local_sem.at[2 + g]
        ).wait()
        products(g, a)
        remote(
            tc_hbm.at[:, chunks * (1 - a) + g],
            s_buf.at[g, pl.ds(half * (1 - a), half)],
            S_IN + g,
            twin,
        ).wait_recv()
        products(g, 1 - a)
        add_gram()
        response[...] = jnp.dot(kron[...], partner[...], preferred_element_type=F32).astype(BF16)
        s_t[...] = s_buf[g].reshape(tall, W).T
        for c0, c1, k0, k1 in TILES + ((8, 9, 4, 9),):
            cols = pl.ds(c0 * B, (c1 - c0) * B)
            rows = pl.ds(k0 * B, (k1 - k0) * B)
            terms[rows, cols] += jnp.dot(s_t[rows, :], response[:, cols], preferred_element_type=F32)
        return carry

    lax.fori_loop(0, chunks, step, 0)

    def own_terms(p, run, d, cj, n=1):
        k = d + 4
        return terms[pl.ds(k * B + run * (B // 2) + p * RUN, RUN), pl.ds((cj + d) * B, n * B)] * keep[k]

    def mates(p, run, slot, cj):
        return pair_in[slot, pl.ds((2 * p + run) * RUN, RUN), pl.ds(cj * B, B)].astype(F32)

    def piece(p):
        return pl.ds(2 * p * RUN, 2 * RUN)

    gpair = [[None] * 4 for _ in range(PIECES)]
    for p in range(PIECES):
        for q in (0, 3, 1, 2):
            c0, n = pair_cols[q]
            cols = pl.ds(c0 * B, n * B)
            for run in (0, 1):
                pair_out[q, pl.ds((2 * p + run) * RUN, RUN), cols] = own_terms(p, run, 2 * q - 3, c0, n).astype(BF16)
            gpair[p][q] = remote(
                pair_out.at[q, piece(p), cols],
                pair_in.at[q + core, piece(p), cols],
                GPAIR + 4 * p + q,
                mate,
            )
            gpair[p][q].start()

    folded = jnp.where(same_row, gram[...], 0.0).reshape(naux, ROWS, tall).sum(1)
    polar = jnp.dot(folded, pick, preferred_element_type=F32, precision=lax.Precision.HIGHEST)
    square_row = lax.broadcasted_iota(jnp.int32, (naux, B), 0)
    square_lane = lax.broadcasted_iota(jnp.int32, (naux, B), 1)
    screen_lane = jnp.sum(jnp.where(square_row == square_lane, screen_all, 0.0), axis=0, keepdims=True)
    polar = polar * screen_all * screen_lane
    packed = polar[:8]
    for n in range(1, naux // 8):
        packed = packed + pltpu.roll(polar[8 * n : 8 * n + 8], n * naux, 1)
    pol_out[0] = packed
    pol_copies = []
    for r, group in enumerate(groups):
        first = sum(len(g) for g in groups[:r])
        pol_copies.append(
            [
                remote(pol_out.at[r], pol_in.at[first + n], POLAR + first + n, device)
                for n, device in enumerate(group)
            ]
        )

    def polar_start(r):
        for copy in pol_copies[r]:
            copy.start()

    def polar_round(r):
        for copy in pol_copies[r]:
            copy.wait_recv()
        first = sum(len(g) for g in groups[:r])
        value = pol_out[r] + pol_in[first]
        if len(groups[r]) == 3:
            value = value + (pol_in[first + 1] + pol_in[first + 2])
        pol_out[r + 1] = value
        if r + 1 < len(groups):
            polar_start(r + 1)

    ahead = list(range(len(groups) - 1))

    def advance():
        if ahead:
            polar_round(ahead.pop(0))

    polar_start(0)
    gup2, gdown2, gup1, gdown1, gaux = [], [], [], [], []
    for p in range(PIECES):
        for q in (0, 3, 1, 2):
            gpair[p][q].wait_recv()
        for run in (0, 1):
            at = pl.ds((2 * p + run) * RUN, RUN)
            for c in range(6):
                part = mates(p, run, 4, c)
                if c < 5:
                    part = part + own_terms(p, run, 4, c)
                out2[0, at, pl.ds(c * B, B)] = part.astype(BF16)
        gup2.append(PerCore(out2.at[0, piece(p)], in2.at[0, piece(p)], GUP2 + p, up, ((0, 6), (0, 5))))
        gup2[p].start()
        for run in (0, 1):
            at = pl.ds((2 * p + run) * RUN, RUN)
            for c in range(6):
                part = mates(p, run, 0, c + 3)
                if c >= 1:
                    part = part + own_terms(p, run, -4, c + 3)
                out2[1, at, pl.ds(c * B, B)] = part.astype(BF16)
        gdown2.append(PerCore(out2.at[1, piece(p)], in2.at[1, piece(p)], GDOWN2 + p, down, ((1, 5), (0, 6))))
        gdown2[p].start()

    advance()

    for p in range(PIECES):
        for run in (0, 1):
            for c in range(SLOTS):
                total[run, pl.ds(p * RUN, RUN), pl.ds(c * B, B)] = mates(p, run, 2, c) + own_terms(p, run, 0, c)
    aux_out[...] = total[1 - a].astype(BF16)
    gaux.append(remote(aux_out, aux_in, GAUX, twin))
    gaux[0].start()

    def last_hop(way, number, p, near, far):
        copies = []
        for kind, device in enumerate((near, far)):
            copies.append(
                PerCore(
                    out1.at[way, p, device[1]],
                    in1.at[way, kind, p],
                    number + 2 * p + kind,
                    device,
                    (((0, 8), (0, 7)), ((1, 7), (0, 8)))[way],
                )
            )
            copies[kind].start()
        return copies

    for p in range(PIECES):
        gup2[p].wait_recv()
        for run in (0, 1):
            at = pl.ds((2 * p + run) * RUN, RUN)
            for c in range(8):
                part = mates(p, run, 3, c)
                if c < 7:
                    part = part + own_terms(p, run, 2, c)
                if c < 6:
                    part = part + in2[0, at, pl.ds(c * B, B)].astype(F32)
                out1[0, p, run, :, pl.ds(c * B, B)] = part.astype(BF16)
        gup1.append(last_hop(0, GUP1, p, up, up_twin))
        gdown2[p].wait_recv()
        for run in (0, 1):
            at = pl.ds((2 * p + run) * RUN, RUN)
            for c in range(8):
                part = mates(p, run, 1, c + 1)
                if c >= 1:
                    part = part + own_terms(p, run, -2, c + 1)
                if c >= 2:
                    part = part + in2[1, at, pl.ds((c - 2) * B, B)].astype(F32)
                out1[1, p, run, :, pl.ds(c * B, B)] = part.astype(BF16)
        gdown1.append(last_hop(1, GDOWN1, p, down, down_twin))
        advance()
    while ahead:
        advance()
    gaux[0].wait_recv()
    for p in range(PIECES):
        for copy in gup1[p] + gdown1[p]:
            copy.wait_recv()
        there = pl.ds(p * RUN, RUN)
        for c in range(SLOTS):
            cols = pl.ds(c * B, B)
            part = total[a, there, cols] + aux_in[there, cols].astype(F32)
            for kind in (0, 1):
                if c < 8:
                    part = part + in1[0, kind, p, :, cols].astype(F32)
                if c >= 1:
                    part = part + in1[1, kind, p, :, pl.ds((c - 1) * B, B)].astype(F32)
            grad_ref[there, cols] = part * (keep[c] * scale_grad)
    polar_round(len(groups) - 1)
    packed = pol_out[len(groups)] * scale_pol
    for n in range(half // 8):
        here = [pltpu.roll(packed, (B - (n + slab * half // 8) * naux) % B, 1) for slab in (0, 1)]
        pol_ref[pl.ds(8 * n, 8), :] = jnp.where(a == 0, here[0], here[1])[:, :naux]

    info_copy.wait_send()
    for g in range(chunks):
        slab_out(g).wait_send()
    sent = [up1, down1, up2, down2] + pair_copies + gup2 + gdown2 + gaux
    for copy in sent + [copy for group in gpair + gup1 + gdown1 + pol_copies for copy in group]:
        copy.wait_send()


def body(occupied, virtual, three_centre, kern, profile, atom_map):
    nchain = lax.axis_size("chain")
    half = three_centre.shape[0]
    naux = kern.shape[1]
    chunks = (B // 2) // ROWS
    tall = naux * ROWS
    polars = 5 + 3 * (nchain >= 64) + (nchain >= 16)
    rounds = 3 + (nchain >= 64) + (nchain >= 16)
    slabs = three_centre.reshape(half, B // ROWS, ROWS, W)
    hbm = pl.BlockSpec(memory_space=pltpu.HBM)
    vmem = pl.BlockSpec(memory_space=pltpu.VMEM)
    grad, pol = pl.pallas_call(
        functools.partial(
            kernel,
            nchain,
            naux,
            nchain // 4,
            1.0 / math.sqrt(B * naux),
            1.0 / math.sqrt(B * nchain * W),
        ),
        out_shape=(
            jax.ShapeDtypeStruct((B // 2, W), F32),
            jax.ShapeDtypeStruct((half, naux), F32),
        ),
        in_specs=[hbm] * 6,
        out_specs=(vmem, vmem),
        scratch_shapes=[
            pltpu.VMEM((chunks, naux, ROWS, W), BF16),
            pltpu.VMEM((5, 2, B, W), BF16),
            pltpu.VMEM((4, 2, B, W), BF16),
            pltpu.VMEM((W, W), BF16),
            pltpu.VMEM((W, W), BF16),
            pltpu.VMEM((5 * B, 2 * B), BF16),
            pltpu.VMEM((W, tall), BF16),
            pltpu.VMEM((tall, W), BF16),
            pltpu.VMEM((tall, W), BF16),
            pltpu.VMEM((tall, W), BF16),
            pltpu.VMEM((tall, tall), F32),
            pltpu.VMEM((tall, tall), BF16),
            pltpu.VMEM((2, 2, half, B), F32),
            pltpu.VMEM((W, W), F32),
            pltpu.VMEM((4, B, W), BF16),
            pltpu.VMEM((5, B, W), BF16),
            pltpu.VMEM((2, B, 6 * B), BF16),
            pltpu.VMEM((2, B, 6 * B), BF16),
            pltpu.VMEM((2, PIECES, 2, RUN, 8 * B), BF16),
            pltpu.VMEM((2, 2, PIECES, RUN, 8 * B), BF16),
            pltpu.VMEM((2, B // 2, W), F32),
            pltpu.VMEM((B // 2, W), BF16),
            pltpu.VMEM((B // 2, W), BF16),
            pltpu.VMEM((rounds + 1, 8, B), F32),
            pltpu.VMEM((polars, 8, B), F32),
            pltpu.VMEM((half, naux), BF16),
            pltpu.SMEM((nchain,), jnp.int32),
            pltpu.SMEM((half,), jnp.int32),
            pltpu.SemaphoreType.DMA((POLAR + polars,)),
            pltpu.SemaphoreType.DMA((POLAR + polars,)),
            pltpu.SemaphoreType.DMA((5 + chunks,)),
        ],
        compiler_params=pltpu.CompilerParams(
            collective_id=0, has_side_effects=True, vmem_limit_bytes=VMEM_LIMIT
        ),
        name="rpa",
    )(*[pltpu.with_memory_space_constraint(x, pltpu.HBM) for x in (occupied, virtual, slabs, kern, profile, atom_map)])
    return grad, pol


def solution(mesh):
    placed = (
        P("chain", None),
        P("chain", None),
        P("aux", "chain", None),
        P("aux", None),
        P(),
        P("aux"),
    )
    return jax.shard_map(
        body,
        mesh=mesh,
        in_specs=placed,
        out_specs=(P(("chain", "aux"), None), P("aux", None)),
        check_vma=False,
    )
```
